32 devices in a mesh: pb: 4 (over y, core), an: 8 (over z, x).
Axes of the slice: x: 2, y: 2, z: 4, core: 2. Of those that a mesh axis runs over, the one named last changes fastest.
Arguments:
- child_ids: int32 [512, 256], P(('pb', 'an')), may hold values from 0 to 262143, as said below
- history_ids: int32 [512, 69], P(('pb', 'an')), may hold values from 0 to 262143, as said below
- node_table: bfloat16 [262144, 128], P(('pb', 'an')), may hold values from -6 to 6
- w_first: bfloat16 [256, 512], replicated, may hold values from -0.375 to 0.375
- b_first: float32 [512], replicated, may hold values from -3 to 3
- w_second: bfloat16 [512, 512], replicated, may hold values from -0.25 to 0.25
- b_second: float32 [512], replicated, may hold values from -3 to 3
- w_out: bfloat16 [512], replicated, may hold values from -0.25 to 0.25
Outputs:
- scores: float32 [512, 256], P(('pb', 'an'))
The draws below stay inside these ranges and needn't reach their ends.
Inputs may be any that keep to these rules, and one draw needn't show every extreme that they name: `child_ids`: in each aligned block of 16 queries (the queries of one device), at most 320 of the child ids lie in any one aligned range of 8192 node ids; some range holds exactly 320 in every block. `history_ids`: in each aligned block of 16 queries, at most 35 of the history ids lie in any one aligned range of 8192 node ids, and some range holds exactly 35.
All inputs are finite; a program needn't handle non-finite values.
Results may differ from the reference program's by a relative error of at most 0.0034.
Values may be sent and summed in bfloat16 or wider, within the bound.
No kernel may reach another device: no remote copies, remote signals or barrier semaphores. Data moves between devices by JAX's collectives and lax.ppermute only.
A program may use at most 64 MiB of HBM per device.

```python
import jax
import jax.numpy as jnp
from jax import lax

E = 128
HID = 512
K = 256
HIST = 69
Q_DEV = 16
NODES_DEV = 8192
QUERIES = 512
NODES = 262144


def shuffle_blocks(key, owners):
    keys = jax.random.split(key, owners.shape[0])
    return jax.vmap(lambda single, row: jax.random.permutation(single, row))(keys, owners)


def draw_child_ids(key, part):
    devices = NODES // NODES_DEV
    row_count = Q_DEV * K
    hot_count = max(1, devices // 8)
    capacity = 5 * row_count // (2 * devices)
    cold_count = devices - hot_count
    order = jax.random.permutation(jax.random.fold_in(key, 11), devices)
    places = jnp.arange(row_count)[None, :]
    shifts = jax.random.randint(jax.random.fold_in(key, 12), (devices, 1), 0, cold_count)
    cold_rank = hot_count + (places - hot_count * capacity + shifts) % cold_count
    ranking = jnp.where(places < hot_count * capacity, places // capacity, cold_rank)
    owners = shuffle_blocks(jax.random.fold_in(key, 13), order[ranking])
    offsets = jax.random.randint(jax.random.fold_in(key, 14), (devices, row_count), 0, NODES_DEV)
    return (owners * NODES_DEV + offsets).reshape(devices * Q_DEV, K).astype(jnp.int32)


def draw_history_ids(key, part):
    devices = NODES // NODES_DEV
    row_count = Q_DEV * HIST
    shifts = jax.random.randint(jax.random.fold_in(key, 21), (devices, 1), 0, devices)
    owners = (jnp.arange(row_count)[None, :] + shifts) % devices
    owners = shuffle_blocks(jax.random.fold_in(key, 22), owners)
    offsets = jax.random.randint(jax.random.fold_in(key, 23), (devices, row_count), 0, NODES_DEV)
    return (owners * NODES_DEV + offsets).reshape(devices * Q_DEV, HIST).astype(jnp.int32)


def levels(stream_key, shape, cuts, low, high):
    loudness, own = 1.0, jax.random.fold_in(stream_key, 6)
    for dim, shards_of in cuts:
        steps = jnp.exp(jax.random.uniform(jax.random.fold_in(own, dim), (shards_of,), jnp.float32, low / len(cuts), high / len(cuts)))
        loudness = loudness * jnp.repeat(steps, shape[dim] // shards_of).reshape([-1 if axis == dim else 1 for axis in range(len(shape))])
    return loudness


def scatter_about(key, extent, deviation, bound, cuts=(), held_as=jnp.bfloat16):
    entries = jax.random.normal(key, extent, jnp.float32) * deviation
    if len(cuts) > 0:
        entries = levels(key, extent, cuts, -0.22, 0.18) * entries
    return jnp.clip(entries, min=-bound, max=bound).astype(held_as)


def setup_inputs(seed: int = 0) -> dict:
    splits = jax.random.split(jax.random.key(seed), 9)
    child_ids = draw_child_ids(jax.random.fold_in(splits[8], 71), 0)
    history_ids = draw_history_ids(jax.random.fold_in(splits[8], 71), 0)
    node_table = scatter_about(splits[2], (NODES, E), 1.0, 6.0, ((0, 32),))
    w_first = scatter_about(splits[3], (2 * E, HID), (2 * E) ** -0.5, 0.375)
    b_first = scatter_about(splits[4], (HID,), 0.5, 3.0, (), jnp.float32)
    w_second = scatter_about(splits[5], (HID, HID), HID ** -0.5, 0.25)
    b_second = scatter_about(splits[6], (HID,), 0.5, 3.0, (), jnp.float32)
    w_out = scatter_about(splits[7], (HID,), HID ** -0.5, 0.25)
    return dict(child_ids=child_ids, history_ids=history_ids, node_table=node_table, w_first=w_first, b_first=b_first, w_second=w_second, b_second=b_second, w_out=w_out)


def reference(child_ids, history_ids, node_table, w_first, b_first, w_second, b_second, w_out):
    def score_block(pair):
        kid_ids, past_ids = pair
        child_rows = jnp.take(node_table, kid_ids, axis=0).astype(jnp.float32)
        past_rows = jnp.take(node_table, past_ids, axis=0).astype(jnp.float32)
        logits = jnp.einsum("qhe,qke->qhk", past_rows, child_rows) * (E ** -0.5)
        attend = (jax.nn.sigmoid(logits) * (HIST ** -0.5)).astype(jnp.bfloat16)
        pooled = jnp.einsum("qhk,qhe->qke", attend.astype(jnp.float32), past_rows).astype(jnp.bfloat16)
        joined = jnp.concatenate([child_rows.astype(jnp.bfloat16), pooled], axis=-1).reshape(-1, 2 * E)
        first = jax.nn.relu(jnp.dot(joined, w_first, preferred_element_type=jnp.float32) + b_first).astype(jnp.bfloat16)
        second = jax.nn.relu(jnp.dot(first, w_second, preferred_element_type=jnp.float32) + b_second).astype(jnp.bfloat16)
        result = jnp.dot(second, w_out, preferred_element_type=jnp.float32)
        return result.reshape(kid_ids.shape[0], K)

    blocks = QUERIES // Q_DEV
    pieces = lax.map(score_block, (child_ids.reshape(blocks, Q_DEV, K), history_ids.reshape(blocks, Q_DEV, HIST)))
    return pieces.reshape(QUERIES, K)
```

```python
import jax
import jax.numpy as jnp
from jax import lax
from jax.sharding import PartitionSpec as P


def rank_within(owners, groups):
    total = owners.shape[0]
    block = 128
    padding = -total % block
    padded = jnp.concatenate([owners, jnp.full((padding,), -1, jnp.int32)])
    hits = (padded[:, None] == jnp.arange(groups, dtype=jnp.int32)[None, :]).astype(jnp.float32)
    hits = hits.reshape((total + padding) // block, block, groups)
    lower = (jnp.arange(block)[:, None] > jnp.arange(block)[None, :]).astype(jnp.float32)
    inside = jnp.einsum("ij,bjc->bic", lower, hits)
    totals = jnp.sum(hits, axis=1)
    before = jnp.cumsum(totals, axis=0) - totals
    ranking = jnp.sum((inside + before[:, None, :]) * hits, axis=2).reshape(total + padding)
    return ranking[:total].astype(jnp.int32)


def place(owners, ranks, offsets, groups, slots):
    hit = owners[:, None] == jnp.arange(groups, dtype=jnp.int32)[None, :]
    high = jnp.where(hit, (offsets // 256)[:, None], 0).astype(jnp.bfloat16)
    low = jnp.where(hit, (offsets % 256)[:, None], 0).astype(jnp.bfloat16)
    spot = (ranks[:, None] == jnp.arange(slots, dtype=jnp.int32)[None, :]).astype(jnp.bfloat16)
    digits = jnp.einsum("io,is->os", jnp.concatenate([high, low], axis=1), spot, preferred_element_type=jnp.float32)
    return digits[:groups].astype(jnp.int32) * 256 + digits[groups:].astype(jnp.int32)


def body(child_ids, history_ids, node_table, w_first, b_first, w_second, b_second, w_out):
    queries, children = child_ids.shape
    history = history_ids.shape[1]
    shard_rows, width = node_table.shape
    peers = lax.axis_size(("pb", "an"))
    row_count = queries * children
    past_count = queries * history
    capacity = 5 * row_count // (2 * peers)
    past_cap = (past_count + peers - 1) // peers
    past_cap += -(capacity + past_cap) % 8
    slots = capacity + past_cap
    table_slots = peers * slots
    kid_flat = child_ids.reshape(row_count)
    past_flat = history_ids.reshape(past_count)
    kid_owner = kid_flat // shard_rows
    past_owner = past_flat // shard_rows
    kid_rank = rank_within(kid_owner, peers)
    past_rank = rank_within(past_owner, peers)
    kid_slot = kid_owner * slots + kid_rank
    past_slot = past_owner * slots + capacity + past_rank
    total = row_count + past_count
    all_slots = jnp.concatenate([kid_slot, past_slot])
    wanted = jnp.concatenate(
        [
            place(kid_owner, kid_rank, kid_flat % shard_rows, peers, capacity),
            place(past_owner, past_rank, past_flat % shard_rows, peers, past_cap),
        ],
        axis=1,
    )
    asked = lax.all_to_all(wanted, ("pb", "an"), split_axis=0, concat_axis=0, tiled=True)
    rows = node_table.at[asked.reshape(table_slots)].get(mode="promise_in_bounds")
    fetched = lax.all_to_all(
        rows.reshape(peers, slots, width), ("pb", "an"), split_axis=0, concat_axis=0, tiled=True
    )
    fetched = fetched.reshape(table_slots, width)
    picked = fetched.at[all_slots].get(mode="promise_in_bounds")
    child_rows = picked[:row_count].reshape(queries, children, width)
    past_rows = picked[row_count:total].reshape(queries, history, width)
    logits = jnp.einsum(
        "qhe,qke->qhk", past_rows, child_rows, preferred_element_type=jnp.float32
    ) * width ** (-0.5)
    attend = (jax.nn.sigmoid(logits) * history ** (-0.5)).astype(jnp.bfloat16)
    pooled = jnp.einsum(
        "qhk,qhe->qke", attend, past_rows, preferred_element_type=jnp.float32
    ).astype(jnp.bfloat16)
    joined = jnp.concatenate([child_rows, pooled], axis=-1).reshape(row_count, 2 * width)
    first = jax.nn.relu(
        jnp.dot(joined, w_first, preferred_element_type=jnp.float32) + b_first
    ).astype(jnp.bfloat16)
    second = jax.nn.relu(
        jnp.dot(first, w_second, preferred_element_type=jnp.float32) + b_second
    ).astype(jnp.bfloat16)
    result = jnp.dot(second, w_out, preferred_element_type=jnp.float32)
    return result.reshape(queries, children)


def solution(mesh):
    placed = (
        P(("pb", "an"), None),
        P(("pb", "an"), None),
        P(("pb", "an"), None),
        P(),
        P(),
        P(),
        P(),
        P(),
    )
    return jax.shard_map(
        body, mesh=mesh, in_specs=placed, out_specs=P(("pb", "an"), None), check_vma=False
    )
```

```python
import jax
import jax.numpy as jnp
from jax import lax
from jax.experimental import pallas as pl
from jax.experimental.pallas import tpu as pltpu
from jax.sharding import Mesh
from jax.sharding import PartitionSpec as P

AXES = ("pb", "ah", "al")
HALF = ("pb", "al")
BLOCK = 512


def rounded(n, m):
    return -(-n // m) * m


def unroll_of(n, most=64):
    return max(u for u in range(1, most + 1) if n % u == 0)


def rank_within(owners, groups):
    total = owners.shape[0]
    block = 128
    padding = -total % block
    padded = jnp.concatenate([owners, jnp.full((padding,), -1, jnp.int32)])
    hits = (padded[:, None] == jnp.arange(groups, dtype=jnp.int32)[None, :]).astype(jnp.float32)
    hits = hits.reshape((total + padding) // block, block, groups)
    lower = (jnp.arange(block)[:, None] > jnp.arange(block)[None, :]).astype(jnp.float32)
    inside = jnp.einsum("ij,bjc->bic", lower, hits)
    totals = jnp.sum(hits, axis=1)
    before = jnp.cumsum(totals, axis=0) - totals
    ranking = jnp.sum((inside + before[:, None, :]) * hits, axis=2).reshape(total + padding)
    return ranking[:total].astype(jnp.int32)


def place(owners, ranks, offsets, groups, slots):
    hit = owners[:, None] == jnp.arange(groups, dtype=jnp.int32)[None, :]
    high = jnp.where(hit, (offsets // 256)[:, None], 0).astype(jnp.bfloat16)
    low = jnp.where(hit, (offsets % 256)[:, None], 0).astype(jnp.bfloat16)
    spot = (ranks[:, None] == jnp.arange(slots, dtype=jnp.int32)[None, :]).astype(jnp.bfloat16)
    digits = jnp.einsum("io,is->os", jnp.concatenate([high, low], axis=1), spot, preferred_element_type=jnp.float32)
    return digits[:groups].astype(jnp.int32) * 256 + digits[groups:].astype(jnp.int32)


VMEM = pl.BlockSpec(memory_space=pltpu.VMEM)
SMEM = pl.BlockSpec(memory_space=pltpu.SMEM)


def widen(src, dst, rows, at=0, step=128):
    def go(i, c):
        dst[pl.ds(at + i * step, step), :] = src[pl.ds(i * step, step), :].astype(jnp.float32)
        return c

    step = unroll_of(rows // 8, step // 8) * 8
    lax.fori_loop(0, rows // step, go, 0)


def narrow(src, dst, rows, step=128):
    def go(i, c):
        dst[pl.ds(i * step, step), :] = src[pl.ds(i * step, step), :].astype(jnp.bfloat16)
        return c

    step = unroll_of(rows // 8, step // 8) * 8
    lax.fori_loop(0, rows // step, go, 0)


def gather_slabs(asked, order, table, shifts, capacity, stride, past_half, peers, al_n):
    width = table.shape[1]
    slab = 2 * capacity
    unroll = unroll_of(capacity)
    per = capacity // unroll

    def kernel(order_ref, asked_ref, table_ref, *rest):
        outs, wide, spare = rest[:-2], rest[-2], rest[-1]
        widen(table_ref, wide, table_ref.shape[0])
        if past_half:
            pasts, outs = outs[0], outs[1:]

            def past(d, c):
                at = d * stride + capacity
                rows = [wide[pl.ds(asked_ref[at + i], 1), :] for i in range(past_half)]
                mate = d + al_n * (1 - 2 * ((d // al_n) % 2))
                for i, row in enumerate(rows):
                    spare[pl.ds(d * 2 * past_half + i, 1), :] = row
                for i, row in enumerate(rows):
                    spare[pl.ds((mate * 2 + 1) * past_half + i, 1), :] = row
                return c

            lax.fori_loop(0, peers, past, 0)
            narrow(spare, pasts, peers * 2 * past_half)
        for out, shift in zip(outs, shifts):

            def child(t, c, shift=shift):
                at = order_ref[2 * shift + t // per] + (t % per) * unroll
                rows = [wide[pl.ds(asked_ref[at + i], 1), :] for i in range(unroll)]
                for i, row in enumerate(rows):
                    spare[pl.ds(t * unroll + i, 1), :] = row
                return c

            lax.fori_loop(0, 2 * per, child, 0)
            narrow(spare, out, slab)

    shapes = [jax.ShapeDtypeStruct((slab, width), table.dtype)] * len(shifts)
    spare_rows = slab
    if past_half:
        shapes = [jax.ShapeDtypeStruct((peers * 2 * past_half, width), table.dtype)] + shapes
        spare_rows = max(slab, peers * 2 * past_half)
    return pl.pallas_call(
        kernel,
        out_shape=shapes,
        in_specs=[SMEM, SMEM, VMEM],
        out_specs=[VMEM] * len(shapes),
        scratch_shapes=[
            pltpu.VMEM(table.shape, jnp.float32),
            pltpu.VMEM((spare_rows, width), jnp.float32),
        ],
        name="gather_past" if past_half else "gather_slabs",
    )(order, asked, table)


def arrange_past(slots, fetched, queries, history, lanes):
    rows, width = fetched.shape

    def kernel(slot_ref, in_ref, out_ref, wide, spare):
        widen(in_ref, wide, rows)
        spare[...] = jnp.zeros(spare.shape, jnp.float32)

        def one(q, c):
            for lo in range(0, history, 35):
                part = range(lo, min(lo + 35, history))
                vals = [wide[pl.ds(slot_ref[q * history + h], 1), :] for h in part]
                for h, val in zip(part, vals):
                    spare[pl.ds(h, 1), :] = val
            out_ref[pl.ds(pl.multiple_of(q * lanes, lanes), lanes), :] = spare[...].astype(jnp.bfloat16)
            return c

        lax.fori_loop(0, queries, one, 0)

    return pl.pallas_call(
        kernel,
        out_shape=jax.ShapeDtypeStruct((queries * lanes, width), fetched.dtype),
        in_specs=[SMEM, VMEM],
        out_specs=VMEM,
        scratch_shapes=[pltpu.VMEM((rows, width), jnp.float32), pltpu.VMEM((lanes, width), jnp.float32)],
        name="arrange_past",
    )(slots, fetched)


def score_rows(segments, bases, rel, slabs, past, w_first, b_first, w_second, b_second, w_out, history, lanes):
    queries, children = rel.shape
    slab, width = slabs[0].shape
    parts = len(slabs)
    hidden = w_second.shape[0]
    longest = queries * children // 2 + children
    longest = rounded(queries * children + queries * 8, BLOCK)
    per_block = BLOCK // 128
    quick = 3
    group = 4

    def kernel(seg_ref, base_ref, rel_ref, past_ref, w1, b1, w2, b2, wo, *rest):
        slab_refs, out_ref = rest[:parts], rest[parts]
        wide, rows, pool, line, g0, g1, g2 = rest[parts + 1 :]
        for i, ref in enumerate(slab_refs):
            widen(ref, wide, slab, at=i * slab)
        spots = lax.broadcasted_iota(jnp.int32, (8, width), 0)

        def segment(t, c):
            src = seg_ref[t]
            dst = seg_ref[queries * parts + t]
            count = seg_ref[2 * queries * parts + t]
            chunks = [wide[pl.ds(src + 8 * i, 8), :] for i in range(quick)]
            for i, chunk in enumerate(chunks):
                pltpu.store(rows.at[pl.ds(dst + 8 * i, 8), :], chunk, mask=spots < count - 8 * i)

            def more(i, c):
                pltpu.store(
                    rows.at[pl.ds(dst + 8 * i, 8), :],
                    wide[pl.ds(src + 8 * i, 8), :],
                    mask=spots < count - 8 * i,
                )
                return c

            lax.fori_loop(quick, (count + 7) // 8, more, 0)
            return c

        lax.fori_loop(0, queries * parts, segment, 0)

        def attend(g, c):
            for i in range(group):
                q = g * group + i
                base = pl.multiple_of(base_ref[q], 8)
                kids = rows[pl.ds(base, children), :].astype(jnp.bfloat16)
                own = past_ref[pl.ds(pl.multiple_of(q * lanes, lanes), lanes), :]
                logits = lax.dot_general(kids, own, (((1,), (1,)), ((), ())), preferred_element_type=jnp.float32)
                logits = logits * width ** (-0.5)
                share = (jax.nn.sigmoid(logits) * history ** (-0.5)).astype(jnp.bfloat16)
                pool[pl.ds(base, children), :] = jnp.dot(share, own, preferred_element_type=jnp.float32)
            return c

        lax.fori_loop(0, queries // group, attend, 0)

        def dense(b, c):
            at = pl.multiple_of(b * BLOCK, BLOCK)
            kids = rows[pl.ds(at, BLOCK), :].astype(jnp.bfloat16)
            pooled = pool[pl.ds(at, BLOCK), :].astype(jnp.bfloat16)
            joined = jnp.concatenate([kids, pooled], axis=1)
            first = jnp.dot(joined, w1[...], preferred_element_type=jnp.float32) + b1[...]
            first = jnp.maximum(first, 0.0).astype(jnp.bfloat16)
            second = jnp.dot(first, w2[...], preferred_element_type=jnp.float32) + b2[...]
            second = jnp.maximum(second, 0.0).astype(jnp.bfloat16)
            out = lax.dot_general(wo[...], second, (((1,), (1,)), ((), ())), preferred_element_type=jnp.float32)
            for i in range(per_block):
                line[pl.ds(b * per_block + i, 1), :] = out[0:1, i * 128 : (i + 1) * 128]
            return c

        lax.fori_loop(0, (base_ref[queries] + BLOCK - 1) // BLOCK, dense, 0)
        for q in range(queries):
            at = base_ref[q] // 128
            for i, ref in enumerate((g0, g1, g2)):
                ref[q : q + 1, :] = line[pl.ds(at + i, 1), :]
        for q in range(0, queries, 8):
            for k in range(0, children, 128):
                spot = rel_ref[q : q + 8, k : k + 128]
                lane = spot & 127
                took = [jnp.take_along_axis(ref[q : q + 8, :], lane, axis=1) for ref in (g0, g1, g2)]
                out_ref[q : q + 8, k : k + 128] = jnp.where(
                    spot < 128, took[0], jnp.where(spot < 256, took[1], took[2])
                )

    wide_rows = parts * slab + 8 * quick
    return pl.pallas_call(
        kernel,
        out_shape=jax.ShapeDtypeStruct((queries, children), jnp.float32),
        in_specs=[SMEM, SMEM] + [VMEM] * (7 + parts),
        out_specs=VMEM,
        scratch_shapes=[
            pltpu.VMEM((wide_rows, width), jnp.float32),
            pltpu.VMEM((longest + children, width), jnp.float32),
            pltpu.VMEM((longest + children, width), jnp.float32),
            pltpu.VMEM((rounded(longest // 128 + 3, 8), 128), jnp.float32),
        ]
        + [pltpu.VMEM((queries, 128), jnp.float32)] * 3,
        name="score_rows",
    )(
        segments,
        bases,
        rel,
        past,
        w_first,
        b_first.reshape(1, hidden),
        w_second,
        b_second.reshape(1, hidden),
        jnp.broadcast_to(w_out[None, :], (8, hidden)),
        *slabs,
    )


def body(child_ids, history_ids, node_table, w_first, b_first, w_second, b_second, w_out):
    queries, children = child_ids.shape
    history = history_ids.shape[1]
    shard_rows, width = node_table.shape
    pb_n, al_n = lax.axis_size("pb"), lax.axis_size("al")
    peers, near = 2 * pb_n * al_n, pb_n * al_n
    pb, ah, al = (lax.axis_index(a) for a in AXES)
    here = pb * al_n + al
    row_count = queries * children
    past_count = queries * history
    capacity = 5 * row_count // (2 * peers)
    past_cap = (past_count + peers - 1) // peers
    past_half = rounded(past_cap, 4)
    stride = rounded(capacity + past_half, 128)
    power = near & (near - 1) == 0

    kid_flat = child_ids.reshape(row_count)
    past_flat = history_ids.reshape(past_count)
    kid_owner = kid_flat // shard_rows
    past_owner = past_flat // shard_rows
    kid_rank = rank_within(kid_owner, peers)
    past_rank = rank_within(past_owner, peers)
    wanted = jnp.concatenate(
        [
            place(kid_owner, kid_rank, kid_flat % shard_rows, peers, capacity),
            place(past_owner, past_rank, past_flat % shard_rows, peers, stride - capacity),
        ],
        axis=1,
    )
    asked = lax.all_to_all(wanted.reshape(peers, 1, stride), AXES, split_axis=0, concat_axis=0, tiled=True)
    asked = asked.reshape(peers * stride)

    shifts = jnp.arange(near, dtype=jnp.int32)
    target = (here ^ shifts) if power else (here + shifts) % near
    lists = (target // al_n) * (2 * al_n) + target % al_n
    order = jnp.stack([lists + ah * al_n, lists + (1 - ah) * al_n], axis=1).reshape(2 * near) * stride

    pairs = [(i, (i ^ s) if power else (i + s) % near) for s in range(near) for i in range(near)]
    steps = sorted(range(near), key=lambda s: (s == 0, -bin(s).count("1"), -s))
    first_cut = max(1, near // 8)
    second_cut = near // 2
    waves = [steps[:first_cut], steps[first_cut:second_cut], steps[second_cut:]]
    slabs = [None] * near
    for number, wave in enumerate(waves):
        outs = gather_slabs(
            asked, order, node_table, wave, capacity, stride, past_half if number == 0 else 0, peers, al_n
        )
        if number == 0:
            past_out, outs = outs[0], outs[1:]
            past_in = lax.all_to_all(
                past_out.reshape(peers, 2 * past_half, width), AXES, split_axis=0, concat_axis=0, tiled=True
            ).reshape(peers * 2 * past_half, width)
        for shift, out in zip(wave, outs):
            slabs[shift] = lax.ppermute(out, HALF, pairs[shift * near : (shift + 1) * near]) if shift else out

    ids = jnp.concatenate([child_ids, past_owner.reshape(queries, history), past_rank.reshape(queries, history)], axis=1)
    swap = [(0, 1), (1, 0)]
    mate_ids = lax.ppermute(ids, "ah", swap)
    both = jnp.stack([ids, mate_ids])
    kids = both[:, :, :children]
    owner = kids // shard_rows
    local = (owner // (2 * al_n)) * al_n + owner % al_n
    inside_half = (owner // al_n) % 2 == ah
    part = (local ^ here) if power else (here - local) % near
    part = jnp.where(inside_half, part, near)
    hits = (part.reshape(2 * queries, children)[:, :, None] == jnp.arange(near, dtype=jnp.int32)).astype(jnp.bfloat16)
    lower = (jnp.arange(children)[:, None] > jnp.arange(children)[None, :]).astype(jnp.bfloat16)
    before = jnp.einsum("kj,qjx->qkx", lower, hits, preferred_element_type=jnp.float32)
    counts = jnp.sum(hits.astype(jnp.float32), axis=1).astype(jnp.int32)
    blocked = counts.reshape(2, queries, near)
    starts = (jnp.cumsum(blocked, axis=1) - blocked).reshape(2 * queries, near)
    offsets = jnp.cumsum(counts, axis=1) - counts
    lengths = (jnp.sum(counts, axis=1) + 7) // 8 * 8
    ends = jnp.cumsum(lengths)
    bases = ends - lengths
    spot = jnp.sum((before + offsets.astype(jnp.float32)[:, None, :]) * hits.astype(jnp.float32), axis=2).astype(jnp.int32)
    rel = spot + (bases % 128)[:, None]
    which = (jnp.arange(2 * queries, dtype=jnp.int32) // queries)[:, None]
    source = jnp.arange(near, dtype=jnp.int32)[None, :] * (2 * capacity) + which * capacity + starts
    segments = jnp.concatenate([source.reshape(-1), (bases[:, None] + offsets).reshape(-1), counts.reshape(-1)])
    bases = jnp.concatenate([bases, ends[-1:]])
    own_past, own_rank = both[:, :, children : children + history], both[:, :, children + history :]
    past_slot = own_past * (2 * past_half) + jnp.arange(2, dtype=jnp.int32)[:, None, None] * past_half + own_rank

    lanes = rounded(history, 128)
    past = arrange_past(past_slot.reshape(-1), past_in, 2 * queries, history, lanes)
    scores = score_rows(segments, bases, rel, slabs, past, w_first, b_first, w_second, b_second, w_out, history, lanes)
    back = lax.ppermute(scores[queries:], "ah", swap)
    return jnp.where(inside_half[0], scores[:queries], back)


def solution(mesh):
    pb_n, an_n = mesh.shape["pb"], mesh.shape["an"]
    fine = Mesh(mesh.devices.reshape(pb_n, 2, an_n // 2), AXES)
    rows = P(AXES, None)
    return jax.shard_map(
        body, mesh=fine, in_specs=(rows, rows, rows, P(), P(), P(), P(), P()), out_specs=rows, check_vma=False
    )
```

```python
import jax
import jax.numpy as jnp
from jax import lax
from jax.experimental import pallas as pl
from jax.experimental.pallas import tpu as pltpu
from jax.sharding import Mesh
from jax.sharding import PartitionSpec as P

AXES = ("pb", "ah", "al")
HALF = ("pb", "al")
BLOCK = 512


def rounded(n, m):
    return -(-n // m) * m


def unroll_of(n, most=64):
    return max(u for u in range(1, most + 1) if n % u == 0)


def rank_within(owners, groups):
    total = owners.shape[0]
    block = 128
    padding = -total % block
    padded = jnp.concatenate([owners, jnp.full((padding,), -1, jnp.int32)])
    hits = (padded[:, None] == jnp.arange(groups, dtype=jnp.int32)[None, :]).astype(jnp.float32)
    hits = hits.reshape((total + padding) // block, block, groups)
    lower = (jnp.arange(block)[:, None] > jnp.arange(block)[None, :]).astype(jnp.float32)
    inside = jnp.einsum("ij,bjc->bic", lower, hits)
    totals = jnp.sum(hits, axis=1)
    before = jnp.cumsum(totals, axis=0) - totals
    ranking = jnp.sum((inside + before[:, None, :]) * hits, axis=2).reshape(total + padding)
    return ranking[:total].astype(jnp.int32)


def place(owners, ranks, offsets, groups, slots):
    hit = owners[:, None] == jnp.arange(groups, dtype=jnp.int32)[None, :]
    high = jnp.where(hit, (offsets // 256)[:, None], 0).astype(jnp.bfloat16)
    low = jnp.where(hit, (offsets % 256)[:, None], 0).astype(jnp.bfloat16)
    spot = (ranks[:, None] == jnp.arange(slots, dtype=jnp.int32)[None, :]).astype(jnp.bfloat16)
    digits = jnp.einsum("io,is->os", jnp.concatenate([high, low], axis=1), spot, preferred_element_type=jnp.float32)
    return digits[:groups].astype(jnp.int32) * 256 + digits[groups:].astype(jnp.int32)


VMEM = pl.BlockSpec(memory_space=pltpu.VMEM)
SMEM = pl.BlockSpec(memory_space=pltpu.SMEM)


def widen(src, dst, rows, at=0, step=128):
    def go(i, c):
        dst[pl.ds(at + i * step, step), :] = src[pl.ds(i * step, step), :].astype(jnp.float32)
        return c

    step = unroll_of(rows // 8, step // 8) * 8
    lax.fori_loop(0, rows // step, go, 0)


def narrow(src, dst, rows, step=128):
    def go(i, c):
        dst[pl.ds(i * step, step), :] = src[pl.ds(i * step, step), :].astype(jnp.bfloat16)
        return c

    step = unroll_of(rows // 8, step // 8) * 8
    lax.fori_loop(0, rows // step, go, 0)


def gather_slabs(asked, order, table, shifts, capacity, stride, past_half, peers, al_n):
    width = table.shape[1]
    slab = 2 * capacity
    unroll = unroll_of(capacity)
    per = capacity // unroll

    def kernel(order_ref, asked_ref, table_ref, *rest):
        outs, wide, spare = rest[:-2], rest[-2], rest[-1]
        widen(table_ref, wide, table_ref.shape[0])
        if past_half:
            pasts, outs = outs[0], outs[1:]

            def past(d, c):
                at = d * stride + capacity
                rows = [wide[pl.ds(asked_ref[at + i], 1), :] for i in range(past_half)]
                mate = d + al_n * (1 - 2 * ((d // al_n) % 2))
                for i, row in enumerate(rows):
                    spare[pl.ds(d * 2 * past_half + i, 1), :] = row
                for i, row in enumerate(rows):
                    spare[pl.ds((mate * 2 + 1) * past_half + i, 1), :] = row
                return c

            lax.fori_loop(0, peers, past, 0)
            narrow(spare, pasts, peers * 2 * past_half)
        for out, shift in zip(outs, shifts):

            def child(t, c, shift=shift):
                at = order_ref[2 * shift + t // per] + (t % per) * unroll
                rows = [wide[pl.ds(asked_ref[at + i], 1), :] for i in range(unroll)]
                for i, row in enumerate(rows):
                    spare[pl.ds(t * unroll + i, 1), :] = row
                return c

            lax.fori_loop(0, 2 * per, child, 0)
            narrow(spare, out, slab)

    shapes = [jax.ShapeDtypeStruct((slab, width), jnp.bfloat16)] * len(shifts)
    spare_rows = slab
    if past_half:
        shapes = [jax.ShapeDtypeStruct((peers * 2 * past_half, width), jnp.bfloat16)] + shapes
        spare_rows = max(slab, peers * 2 * past_half)
    return pl.pallas_call(
        kernel,
        out_shape=shapes,
        in_specs=[SMEM, SMEM, VMEM],
        out_specs=[VMEM] * len(shapes),
        scratch_shapes=[
            pltpu.VMEM(table.shape, jnp.float32),
            pltpu.VMEM((spare_rows, width), jnp.float32),
        ],
        name="gather_past" if past_half else "gather_slabs",
    )(order, asked, table)


def arrange_past(slots, fetched, queries, history, lanes):
    rows, width = fetched.shape

    def kernel(slot_ref, in_ref, out_ref, wide, spare):
        widen(in_ref, wide, rows)
        spare[...] = jnp.zeros(spare.shape, jnp.float32)

        def one(q, c):
            for lo in range(0, history, 35):
                part = range(lo, min(lo + 35, history))
                vals = [wide[pl.ds(slot_ref[q * history + h], 1), :] for h in part]
                for h, val in zip(part, vals):
                    spare[pl.ds(h, 1), :] = val
            out_ref[pl.ds(pl.multiple_of(q * lanes, lanes), lanes), :] = spare[...].astype(jnp.bfloat16)
            return c

        lax.fori_loop(0, queries, one, 0)

    return pl.pallas_call(
        kernel,
        out_shape=jax.ShapeDtypeStruct((queries * lanes, width), fetched.dtype),
        in_specs=[SMEM, VMEM],
        out_specs=VMEM,
        scratch_shapes=[pltpu.VMEM((rows, width), jnp.float32), pltpu.VMEM((lanes, width), jnp.float32)],
        name="arrange_past",
    )(slots, fetched)


def score_rows(segments, bases, rel, slabs, past, w_first, b_first, w_second, b_second, w_out, history, lanes):
    queries, children = rel.shape
    slab, width = slabs[0].shape
    parts = len(slabs)
    hidden = w_second.shape[0]
    total = queries * parts
    batch = 8
    longest = rounded(queries * children + queries * 8, BLOCK)
    per_block = BLOCK // 128
    quick = 3
    group = 4
    half = queries // 2

    def kernel(seg_ref, base_ref, rel_ref, past_ref, w1, b1, w2, b2, wo, *rest):
        slab_refs, out_refs = rest[:parts], rest[parts : parts + 2]
        wide, rows, pool, line, g0, g1, g2 = rest[parts + 2 :]
        for i, ref in enumerate(slab_refs):
            widen(ref, wide, slab, at=i * slab)
        spots = lax.broadcasted_iota(jnp.int32, (8, width), 0)

        def segment(g, c):
            at = [g * batch + i for i in range(batch)]
            src = [seg_ref[t] for t in at]
            dst = [seg_ref[total + t] for t in at]
            count = [seg_ref[2 * total + t] for t in at]
            chunks = [[wide[pl.ds(s + 8 * i, 8), :] for i in range(quick)] for s in src]
            for d, n, chunk in zip(dst, count, chunks):
                for i, part in enumerate(chunk):
                    pltpu.store(rows.at[pl.ds(d + 8 * i, 8), :], part, mask=spots < n - 8 * i)
            most = count[0]
            for n in count[1:]:
                most = jnp.maximum(most, n)

            @pl.when(most > 8 * quick)
            def _():
                for s, d, n in zip(src, dst, count):

                    def more(i, c, s=s, d=d, n=n):
                        pltpu.store(
                            rows.at[pl.ds(d + 8 * i, 8), :], wide[pl.ds(s + 8 * i, 8), :], mask=spots < n - 8 * i
                        )
                        return c

                    lax.fori_loop(quick, (n + 7) // 8, more, 0)

            return c

        lax.fori_loop(0, total // batch, segment, 0)

        def attend(g, c):
            for i in range(group):
                q = g * group + i
                base = pl.multiple_of(base_ref[q], 8)
                kids = rows[pl.ds(base, children), :].astype(jnp.bfloat16)
                own = past_ref[pl.ds(pl.multiple_of(q * lanes, lanes), lanes), :]
                logits = lax.dot_general(kids, own, (((1,), (1,)), ((), ())), preferred_element_type=jnp.float32)
                logits = logits * width ** (-0.5)
                share = (jax.nn.sigmoid(logits) * history ** (-0.5)).astype(jnp.bfloat16)
                pool[pl.ds(base, children), :] = jnp.dot(share, own, preferred_element_type=jnp.float32)
            return c

        lax.fori_loop(0, queries // group, attend, 0)

        def dense(b, c):
            at = pl.multiple_of(b * BLOCK, BLOCK)
            kids = rows[pl.ds(at, BLOCK), :].astype(jnp.bfloat16)
            pooled = pool[pl.ds(at, BLOCK), :].astype(jnp.bfloat16)
            joined = jnp.concatenate([kids, pooled], axis=1)
            first = jnp.dot(joined, w1[...], preferred_element_type=jnp.float32) + b1[...]
            first = jnp.maximum(first, 0.0).astype(jnp.bfloat16)
            second = jnp.dot(first, w2[...], preferred_element_type=jnp.float32) + b2[...]
            second = jnp.maximum(second, 0.0).astype(jnp.bfloat16)
            out = lax.dot_general(wo[...], second, (((1,), (1,)), ((), ())), preferred_element_type=jnp.float32)
            for i in range(per_block):
                line[pl.ds(b * per_block + i, 1), :] = out[0:1, i * 128 : (i + 1) * 128]
            return c

        lax.fori_loop(0, (base_ref[queries] + BLOCK - 1) // BLOCK, dense, 0)
        for q in range(queries):
            at = base_ref[q] // 128
            for i, ref in enumerate((g0, g1, g2)):
                ref[q : q + 1, :] = line[pl.ds(at + i, 1), :]
        for q in range(0, queries, 8):
            for k in range(0, children, 128):
                spot = rel_ref[q : q + 8, k : k + 128]
                lane = spot & 127
                took = [jnp.take_along_axis(ref[q : q + 8, :], lane, axis=1) for ref in (g0, g1, g2)]
                out_ref, at = out_refs[q // half], q % half
                out_ref[at : at + 8, k : k + 128] = jnp.where(
                    spot < 128, took[0], jnp.where(spot < 256, took[1], took[2])
                )

    wide_rows = parts * slab + 8 * quick
    return pl.pallas_call(
        kernel,
        out_shape=[jax.ShapeDtypeStruct((half, children), jnp.float32)] * 2,
        in_specs=[SMEM, SMEM] + [VMEM] * (7 + parts),
        out_specs=[VMEM] * 2,
        scratch_shapes=[
            pltpu.VMEM((wide_rows, width), jnp.float32),
            pltpu.VMEM((longest + children, width), jnp.float32),
            pltpu.VMEM((longest + children, width), jnp.float32),
            pltpu.VMEM((rounded(longest // 128 + 3, 8), 128), jnp.float32),
        ]
        + [pltpu.VMEM((queries, 128), jnp.float32)] * 3,
        name="score_rows",
    )(
        segments,
        bases,
        rel,
        past,
        w_first,
        b_first.reshape(1, hidden),
        w_second,
        b_second.reshape(1, hidden),
        w_out,
        *slabs,
    )


def body(child_ids, history_ids, node_table, w_first, b_first, w_second, b_second, w_out):
    queries, children = child_ids.shape
    history = history_ids.shape[1]
    shard_rows, width = node_table.shape
    pb_n, al_n = lax.axis_size("pb"), lax.axis_size("al")
    peers, near = 2 * pb_n * al_n, pb_n * al_n
    pb, ah, al = (lax.axis_index(a) for a in AXES)
    here = pb * al_n + al
    row_count = queries * children
    past_count = queries * history
    capacity = 5 * row_count // (2 * peers)
    past_cap = (past_count + peers - 1) // peers
    past_half = rounded(past_cap, 4)
    stride = rounded(capacity + past_half, 128)
    power = near & (near - 1) == 0

    kid_flat = child_ids.reshape(row_count)
    past_flat = history_ids.reshape(past_count)
    kid_owner = kid_flat // shard_rows
    past_owner = past_flat // shard_rows
    kid_rank = rank_within(kid_owner, peers)
    past_rank = rank_within(past_owner, peers)
    wanted = jnp.concatenate(
        [
            place(kid_owner, kid_rank, kid_flat % shard_rows, peers, capacity),
            place(past_owner, past_rank, past_flat % shard_rows, peers, stride - capacity),
        ],
        axis=1,
    )
    asked = lax.all_to_all(wanted.reshape(peers, 1, stride), AXES, split_axis=0, concat_axis=0, tiled=True)
    asked = asked.reshape(peers * stride)

    ids = jnp.concatenate([child_ids, past_owner.reshape(queries, history), past_rank.reshape(queries, history)], axis=1)
    swap = [(0, 1), (1, 0)]
    mate_ids = lax.ppermute(ids, "ah", swap)
    shifts = jnp.arange(near, dtype=jnp.int32)
    target = (here ^ shifts) if power else (here + shifts) % near
    lists = (target // al_n) * (2 * al_n) + target % al_n
    order = jnp.stack([lists + ah * al_n, lists + (1 - ah) * al_n], axis=1).reshape(2 * near) * stride

    pairs = [(i, (i ^ s) if power else (i + s) % near) for s in range(near) for i in range(near)]
    steps = sorted(range(1, near), key=lambda s: (-bin(s).count("1"), -s))
    cuts = [0, 3 * near // 16, near // 2, near - 1]
    waves = [steps[a:b] for a, b in zip(cuts, cuts[1:])] + [[0]]
    slabs = [None] * near
    for number, wave in enumerate(waves):
        outs = gather_slabs(
            asked, order, node_table, wave, capacity, stride, past_half if number == 1 else 0, peers, al_n
        )
        if number == 1:
            past_out, outs = outs[0], outs[1:]
            past_in = lax.all_to_all(
                past_out.reshape(peers, 2 * past_half, width), AXES, split_axis=0, concat_axis=0, tiled=True
            ).reshape(peers * 2 * past_half, width)
        if number == len(waves) - 1:
            slabs[0] = outs[0]
            break
        for shift, out in zip(wave, outs):
            slabs[shift] = lax.ppermute(out, HALF, pairs[shift * near : (shift + 1) * near])

    ids, mate_ids, _ = lax.optimization_barrier((ids, mate_ids, slabs[0]))
    both = jnp.stack([ids, mate_ids])
    kids = both[:, :, :children]
    owner = kids // shard_rows
    local = (owner // (2 * al_n)) * al_n + owner % al_n
    inside_half = (owner // al_n) % 2 == ah
    part = (local ^ here) if power else (here - local) % near
    part = jnp.where(inside_half, part, near)
    hits = (part.reshape(2 * queries, children)[:, :, None] == jnp.arange(near, dtype=jnp.int32)).astype(jnp.bfloat16)
    lower = (jnp.arange(children)[:, None] > jnp.arange(children)[None, :]).astype(jnp.bfloat16)
    before = jnp.einsum("kj,qjx->qkx", lower, hits, preferred_element_type=jnp.float32)
    counts = jnp.sum(hits.astype(jnp.float32), axis=1).astype(jnp.int32)
    blocked = counts.reshape(2, queries, near)
    starts = (jnp.cumsum(blocked, axis=1) - blocked).reshape(2 * queries, near)
    offsets = jnp.cumsum(counts, axis=1) - counts
    lengths = (jnp.sum(counts, axis=1) + 7) // 8 * 8
    ends = jnp.cumsum(lengths)
    bases = ends - lengths
    spot = jnp.sum((before + offsets.astype(jnp.float32)[:, None, :]) * hits.astype(jnp.float32), axis=2).astype(jnp.int32)
    rel = spot + (bases % 128)[:, None]
    which = (jnp.arange(2 * queries, dtype=jnp.int32) // queries)[:, None]
    source = jnp.arange(near, dtype=jnp.int32)[None, :] * (2 * capacity) + which * capacity + starts
    segments = jnp.concatenate([source.reshape(-1), (bases[:, None] + offsets).reshape(-1), counts.reshape(-1)])
    bases = jnp.concatenate([bases, ends[-1:]])
    own_past, own_rank = both[:, :, children : children + history], both[:, :, children + history :]
    past_slot = own_past * (2 * past_half) + jnp.arange(2, dtype=jnp.int32)[:, None, None] * past_half + own_rank

    w_last = jnp.broadcast_to(w_out[None, :], (8, w_out.shape[0]))
    mine = inside_half[0].astype(jnp.int32)

    lanes = rounded(history, 128)
    past = arrange_past(past_slot.reshape(-1), past_in, 2 * queries, history, lanes)
    own, lent = score_rows(segments, bases, rel, slabs, past, w_first, b_first, w_second, b_second, w_last, history, lanes)
    back = lax.ppermute(lent, "ah", swap)
    return jnp.where(mine > 0, own, back)


def solution(mesh):
    pb_n, an_n = mesh.shape["pb"], mesh.shape["an"]
    fine = Mesh(mesh.devices.reshape(pb_n, 2, an_n // 2), AXES)
    rows = P(AXES, None)
    return jax.shard_map(
        body, mesh=fine, in_specs=(rows, rows, rows, P(), P(), P(), P(), P()), out_specs=rows, check_vma=False
    )
```

```python
import jax
import jax.numpy as jnp
from jax import lax
from jax.experimental import pallas as pl
from jax.experimental.pallas import tpu as pltpu
from jax.sharding import Mesh
from jax.sharding import PartitionSpec as P

AXES = ("pb", "ah", "al")
HALF = ("pb", "al")
BLOCK = 1024


def rounded(n, m):
    return -(-n // m) * m


def unroll_of(n, most=64):
    return max(u for u in range(1, most + 1) if n % u == 0)


VMEM = pl.BlockSpec(memory_space=pltpu.VMEM)
SMEM = pl.BlockSpec(memory_space=pltpu.SMEM)


def near_by(x):
    return pltpu.with_memory_space_constraint(x, pltpu.VMEM)


def widen(src, dst, rows, at=0, step=128):
    def go(i, c):
        dst[pl.ds(at + i * step, step), :] = src[pl.ds(i * step, step), :].astype(jnp.float32)
        return c

    step = unroll_of(rows // 8, step // 8) * 8
    lax.fori_loop(0, rows // step, go, 0)


def narrow(src, dst, rows, step=128):
    def go(i, c):
        dst[pl.ds(i * step, step), :] = src[pl.ds(i * step, step), :].astype(jnp.bfloat16)
        return c

    step = unroll_of(rows // 8, step // 8) * 8
    lax.fori_loop(0, rows // step, go, 0)


def split(ids, m):
    if m & (m - 1) == 0:
        return ids >> (m.bit_length() - 1), ids & (m - 1)
    return ids // m, ids % m


def iota(shape, axis):
    return lax.broadcasted_iota(jnp.int32, shape, axis)


def ones_where(mask):
    return jnp.where(mask, 1.0, 0.0).astype(jnp.bfloat16)


def exact_dot(a, b):
    return jnp.dot(a.astype(jnp.bfloat16), b.astype(jnp.bfloat16), preferred_element_type=jnp.float32)


def occurrences(keys, groups):
    rows, lanes = keys.shape
    hits = [keys == g for g in range(groups)]
    stack = jnp.concatenate([ones_where(hit) for hit in hits], axis=0)
    before = exact_dot(stack, ones_where(iota((lanes, lanes), 0) < iota((lanes, lanes), 1)))
    totals = exact_dot(stack, jnp.ones((lanes, 128), jnp.bfloat16))
    lane = iota((rows, 128), 1)
    counts = jnp.zeros((rows, 128), jnp.float32)
    for g in range(groups):
        counts = jnp.where(lane == g, totals[g * rows : (g + 1) * rows], counts)
    return hits, [before[g * rows : (g + 1) * rows] for g in range(groups)], counts


def places(hits, before, shifts):
    out = jnp.zeros(hits[0].shape, jnp.float32)
    for g, hit in enumerate(hits):
        out = jnp.where(hit, before[g] + shifts[:, g : g + 1], out)
    return out.astype(jnp.int32)


def build_lists(child_ids, history_ids, shard_rows, peers, capacity, past_half, stride):
    queries, children = child_ids.shape
    history = history_ids.shape[1]
    lanes = rounded(history, 128)
    digit_rows = rounded(2 * peers, 128)

    def kernel(kid_ref, past_ref, want_ref, ids_ref, pad, acc, spot_ref, digit_ref, *scratch):
        pad[...] = jnp.full(pad.shape, -1, jnp.int32)
        pad[:, :history] = past_ref[...]
        strict = ones_where(iota((queries, queries), 0) > iota((queries, queries), 1))
        for source, low, high, (owner_ref, rank_ref, off_ref) in (
            (kid_ref, 0, capacity, scratch[:3]),
            (pad, capacity, stride, scratch[3:]),
        ):
            owner, offset = split(source[...], shard_rows)
            hits, before, counts = occurrences(owner, peers)
            rank = places(hits, before, exact_dot(strict, counts))
            owner_ref[...] = owner
            rank_ref[...] = rank
            off_ref[...] = offset
            if low:
                ids_ref[:, children:] = owner * (2 * past_half) + rank
            else:
                ids_ref[:, :children] = source[...]
            size = source.shape[1]
            if digit_rows > 2 * peers:
                digit_ref[2 * peers :, :] = jnp.zeros((digit_rows - 2 * peers, digit_ref.shape[1]), jnp.bfloat16)

            def query(q, c, low=low, high=high, owner_ref=owner_ref, rank_ref=rank_ref, off_ref=off_ref, size=size):
                at = pl.ds(pl.multiple_of(q * size, size), size)
                hit = iota((peers, size), 0) == owner_ref[pl.ds(q, 1), :]
                offset = off_ref[pl.ds(q, 1), :].astype(jnp.float32)
                upper = jnp.floor(offset * (1.0 / 256.0))
                digit_ref[:peers, at] = jnp.where(hit, upper, 0.0).astype(jnp.bfloat16)
                digit_ref[peers : 2 * peers, at] = jnp.where(hit, offset - 256.0 * upper, 0.0).astype(jnp.bfloat16)
                spot_ref[: high - low, at] = ones_where(iota((high - low, size), 0) == rank_ref[pl.ds(q, 1), :])
                return c

            lax.fori_loop(0, queries, query, 0, unroll=2)
            acc[low:high, :] = lax.dot_general(
                spot_ref[: high - low, : queries * size],
                digit_ref[:, : queries * size],
                (((1,), (1,)), ((), ())),
                preferred_element_type=jnp.float32,
            )
        digits = acc[...].T.astype(jnp.int32)
        wanted = digits[:peers] * 256 + digits[peers : 2 * peers]
        for o in range(peers):
            want_ref[o, 0:1, :] = wanted[o : o + 1, :]

    return pl.pallas_call(
        kernel,
        out_shape=[
            jax.ShapeDtypeStruct((peers, 1, stride), jnp.int32),
            jax.ShapeDtypeStruct((queries, children + lanes), jnp.int32),
        ],
        in_specs=[VMEM, VMEM],
        out_specs=[VMEM, VMEM],
        scratch_shapes=[
            pltpu.VMEM((queries, lanes), jnp.int32),
            pltpu.VMEM((stride, digit_rows), jnp.float32),
            pltpu.VMEM((max(capacity, stride - capacity), queries * max(children, lanes)), jnp.bfloat16),
            pltpu.VMEM((digit_rows, queries * max(children, lanes)), jnp.bfloat16),
        ]
        + [pltpu.VMEM((queries, children), jnp.int32)] * 3
        + [pltpu.VMEM((queries, lanes), jnp.int32)] * 3,
        name="build_lists",
    )(child_ids, history_ids)


def plan_rows(here, ids, mate_ids, shard_rows, children, al_n, near, capacity, past_half):
    half = ids.shape[0]
    queries = 2 * half
    lanes = ids.shape[1] - children

    def kernel(here_ref, ids_ref, mate_ref, seg_ref, base_ref, rel_ref, slot_ref, mine_ref):
        at, side = here_ref[0], here_ref[1]
        kids = jnp.concatenate([ids_ref[:, :children], mate_ref[:, :children]], axis=0)
        owner, _ = split(kids, shard_rows)
        line, spot = split(owner, al_n)
        block, which_half = split(line, 2)
        local = block * al_n + spot
        part = (local ^ at) if near & (near - 1) == 0 else lax.rem(at - local + near, near)
        inside = which_half == side
        mine_ref[...] = inside[:half].astype(jnp.int32)
        hits, before, counts = occurrences(jnp.where(inside, part, near), near)
        row, col = iota((queries, queries), 0), iota((queries, queries), 1)
        lower = row > col
        starts = exact_dot(ones_where(lower & ((row < half) == (col < half))), counts).astype(jnp.int32)
        square = (128, 128)
        offsets = exact_dot(counts, ones_where(iota(square, 0) < iota(square, 1)))
        lengths = exact_dot(counts, jnp.ones(square, jnp.bfloat16)).astype(jnp.int32)
        lengths = (lengths + 7) & -8
        bases = exact_dot(ones_where(lower), lengths.astype(jnp.float32)).astype(jnp.int32)
        rel_ref[...] = places(hits, before, offsets + (bases & 127).astype(jnp.float32))
        mate_rows = iota((queries, 128), 0) >= half
        seg_ref[:queries] = (
            iota((queries, 128), 1) * (2 * capacity) + jnp.where(mate_rows, capacity, 0) + starts
        )
        seg_ref[queries : 2 * queries] = bases + offsets.astype(jnp.int32)
        seg_ref[2 * queries :] = counts.astype(jnp.int32)
        base_ref[:queries] = bases
        base_ref[queries:] = jnp.broadcast_to((bases + lengths)[queries - 1 :], (8, 128))
        slot_ref[:half] = ids_ref[:, children:]
        slot_ref[half:] = mate_ref[:, children:] + past_half

    shapes = [(3 * queries, 128), (queries + 8, 128), (queries, children), (queries, lanes), (half, children)]
    return pl.pallas_call(
        kernel,
        out_shape=[jax.ShapeDtypeStruct(shape, jnp.int32) for shape in shapes],
        in_specs=[SMEM, VMEM, VMEM],
        out_specs=[VMEM] * len(shapes),
        name="plan_rows",
    )(here, ids, near_by(mate_ids))


def gather_slabs(asked, here, table, shifts, capacity, stride, past_half, peers, al_n):
    width = table.shape[1]
    slab = 2 * capacity
    unroll = unroll_of(capacity)
    per = capacity // unroll

    def kernel(here_ref, asked_ref, table_ref, *rest):
        outs, wide, spare = rest[:-2], rest[-2], rest[-1]
        widen(table_ref, wide, table_ref.shape[0])
        if past_half:
            pasts, outs = outs[0], outs[1:]

            def past(d, c):
                at = d * stride + capacity
                rows = [wide[pl.ds(asked_ref[at + i], 1), :] for i in range(past_half)]
                mate = d + al_n * (1 - 2 * lax.rem(lax.div(d, al_n), 2))
                for i, row in enumerate(rows):
                    spare[pl.ds(d * 2 * past_half + i, 1), :] = row
                for i, row in enumerate(rows):
                    spare[pl.ds((mate * 2 + 1) * past_half + i, 1), :] = row
                return c

            lax.fori_loop(0, peers, past, 0)
            narrow(spare, pasts, peers * 2 * past_half)
        near = peers // 2
        at, side = here_ref[0], here_ref[1]
        for out, shift in zip(outs, shifts):
            target = (at ^ shift) if near & (near - 1) == 0 else lax.rem(at + shift, near)
            row = lax.div(target, al_n) * (2 * al_n) + lax.rem(target, al_n)
            own, mate = (row + side * al_n) * stride, (row + (1 - side) * al_n) * stride

            def child(t, c, own=own, mate=mate):
                at = jnp.where(t < per, own, mate - per * unroll) + t * unroll
                rows = [wide[pl.ds(asked_ref[at + i], 1), :] for i in range(unroll)]
                for i, row in enumerate(rows):
                    spare[pl.ds(t * unroll + i, 1), :] = row
                return c

            lax.fori_loop(0, 2 * per, child, 0)
            narrow(spare, out, slab)

    shapes = [jax.ShapeDtypeStruct((slab, width), jnp.bfloat16)] * len(shifts)
    spare_rows = slab
    if past_half:
        shapes = [jax.ShapeDtypeStruct((peers * 2 * past_half, width), jnp.bfloat16)] + shapes
        spare_rows = max(slab, peers * 2 * past_half)
    return pl.pallas_call(
        kernel,
        out_shape=shapes,
        in_specs=[SMEM, SMEM, VMEM],
        out_specs=[VMEM] * len(shapes),
        scratch_shapes=[
            pltpu.VMEM(table.shape, jnp.float32),
            pltpu.VMEM((spare_rows, width), jnp.float32),
        ],
        name="gather_past" if past_half else "gather_slabs",
    )(here, asked, table)


def arrange_past(slots, fetched, queries, history, lanes):
    rows, width = fetched.shape

    def kernel(slot_ref, in_ref, out_ref, wide, spare):
        widen(in_ref, wide, rows)
        spare[...] = jnp.zeros(spare.shape, jnp.float32)

        def one(q, c):
            for lo in range(0, history, 35):
                part = range(lo, min(lo + 35, history))
                vals = [wide[pl.ds(slot_ref[q, h], 1), :] for h in part]
                for h, val in zip(part, vals):
                    spare[pl.ds(h, 1), :] = val
            out_ref[pl.ds(pl.multiple_of(q * lanes, lanes), lanes), :] = spare[...].astype(jnp.bfloat16)
            return c

        lax.fori_loop(0, queries, one, 0)

    return pl.pallas_call(
        kernel,
        out_shape=jax.ShapeDtypeStruct((queries * lanes, width), fetched.dtype),
        in_specs=[SMEM, VMEM],
        out_specs=VMEM,
        scratch_shapes=[pltpu.VMEM((rows, width), jnp.float32), pltpu.VMEM((lanes, width), jnp.float32)],
        name="arrange_past",
    )(slots, near_by(fetched))


def score_rows(segments, bases, rel, slabs, past, w_first, b_first, w_second, b_second, w_out, history, lanes):
    queries, children = rel.shape
    slab, width = slabs[0].shape
    parts = len(slabs)
    hidden = w_second.shape[0]
    batch = min(parts, 16)
    longest = rounded(queries * children + queries * 8, BLOCK)
    per_block = BLOCK // 128
    quick = 3
    group = 16
    half = queries // 2

    def kernel(seg_ref, base_ref, rel_ref, past_ref, w1, b1, w2, b2, wo, *rest):
        slab_refs, out_refs = rest[:parts], rest[parts : parts + 2]
        wide, rows, pool, line, g0, g1, g2 = rest[parts + 2 :]
        for i, ref in enumerate(slab_refs):
            widen(ref, wide, slab, at=i * slab)
        spots = [lax.broadcasted_iota(jnp.int32, (8, width), 0) + 8 * i for i in range(quick)]

        def segment(q, c):
            for x in range(0, parts, batch):
                src, dst, count = ([seg_ref[n * queries + q, x + i] for i in range(batch)] for n in range(3))
                chunks = [[wide[pl.ds(s + 8 * i, 8), :] for i in range(quick)] for s in src]
                for d, n, chunk in zip(dst, count, chunks):
                    for i, part in enumerate(chunk):
                        pltpu.store(rows.at[pl.ds(d + 8 * i, 8), :], part, mask=spots[i] < n)
                most = count[0]
                for n in count[1:]:
                    most = jnp.maximum(most, n)

                @pl.when(most > 8 * quick)
                def _(src=src, dst=dst, count=count):
                    for s, d, n in zip(src, dst, count):

                        def more(i, c, s=s, d=d, n=n):
                            pltpu.store(
                                rows.at[pl.ds(d + 8 * i, 8), :], wide[pl.ds(s + 8 * i, 8), :], mask=spots[0] < n - 8 * i
                            )
                            return c

                        lax.fori_loop(quick, (n + 7) >> 3, more, 0)

            return c

        lax.fori_loop(0, queries, segment, 0)

        def attend(g, c):
            for i in range(group):
                q = g * group + i
                base = pl.multiple_of(base_ref[q, 0], 8)
                kids = rows[pl.ds(base, children), :].astype(jnp.bfloat16)
                own = past_ref[pl.ds(pl.multiple_of(q * lanes, lanes), lanes), :]
                logits = lax.dot_general(kids, own, (((1,), (1,)), ((), ())), preferred_element_type=jnp.float32)
                logits = logits * width ** (-0.5)
                share = (jax.nn.sigmoid(logits) * history ** (-0.5)).astype(jnp.bfloat16)
                pool[pl.ds(base, children), :] = jnp.dot(share, own, preferred_element_type=jnp.float32)
            return c

        lax.fori_loop(0, queries // group, attend, 0)

        last = jnp.broadcast_to(wo[...], (8, hidden))

        def dense(b, c):
            at = pl.multiple_of(b * BLOCK, BLOCK)
            kids = rows[pl.ds(at, BLOCK), :].astype(jnp.bfloat16)
            pooled = pool[pl.ds(at, BLOCK), :].astype(jnp.bfloat16)
            joined = jnp.concatenate([kids, pooled], axis=1)
            first = jnp.dot(joined, w1[...], preferred_element_type=jnp.float32) + b1[...]
            first = jnp.maximum(first, 0.0).astype(jnp.bfloat16)
            second = jnp.dot(first, w2[...], preferred_element_type=jnp.float32) + b2[...]
            second = jnp.maximum(second, 0.0).astype(jnp.bfloat16)
            out = lax.dot_general(last, second, (((1,), (1,)), ((), ())), preferred_element_type=jnp.float32)
            for i in range(per_block):
                line[pl.ds(b * per_block + i, 1), :] = out[0:1, i * 128 : (i + 1) * 128]
            return c

        lax.fori_loop(0, (base_ref[queries, 0] + BLOCK - 1) // BLOCK, dense, 0)
        for q in range(queries):
            at = base_ref[q, 0] // 128
            for i, ref in enumerate((g0, g1, g2)):
                ref[q : q + 1, :] = line[pl.ds(at + i, 1), :]
        for q in range(0, queries, 8):
            for k in range(0, children, 128):
                spot = rel_ref[q : q + 8, k : k + 128]
                lane = spot & 127
                took = [jnp.take_along_axis(ref[q : q + 8, :], lane, axis=1) for ref in (g0, g1, g2)]
                out_ref, at = out_refs[q // half], q % half
                out_ref[at : at + 8, k : k + 128] = jnp.where(
                    spot < 128, took[0], jnp.where(spot < 256, took[1], took[2])
                )

    wide_rows = parts * slab + 8 * quick
    return pl.pallas_call(
        kernel,
        out_shape=[jax.ShapeDtypeStruct((half, children), jnp.float32)] * 2,
        in_specs=[SMEM, SMEM] + [VMEM] * (7 + parts),
        out_specs=[VMEM] * 2,
        scratch_shapes=[
            pltpu.VMEM((wide_rows, width), jnp.float32),
            pltpu.VMEM((longest + children, width), jnp.float32),
            pltpu.VMEM((longest + children, width), jnp.float32),
            pltpu.VMEM((rounded(longest // 128 + 3, 8), 128), jnp.float32),
        ]
        + [pltpu.VMEM((queries, 128), jnp.float32)] * 3,
        name="score_rows",
    )(
        segments,
        bases,
        rel,
        past,
        w_first,
        b_first.reshape(1, hidden),
        w_second,
        b_second.reshape(1, hidden),
        w_out,
        *slabs,
    )


def body(child_ids, history_ids, node_table, w_first, b_first, w_second, b_second, w_out):
    queries, children = child_ids.shape
    history = history_ids.shape[1]
    shard_rows, width = node_table.shape
    pb_n, al_n = lax.axis_size("pb"), lax.axis_size("al")
    peers, near = 2 * pb_n * al_n, pb_n * al_n
    pb, ah, al = (lax.axis_index(a) for a in AXES)
    place = jnp.stack([pb * al_n + al, ah])
    capacity = 5 * queries * children // (2 * peers)
    past_cap = (queries * history + peers - 1) // peers
    past_half = rounded(past_cap, 4)
    stride = rounded(capacity + past_half, 128)
    power = near & (near - 1) == 0

    wanted, ids = build_lists(child_ids, history_ids, shard_rows, peers, capacity, past_half, stride)
    asked = lax.all_to_all(wanted, AXES, split_axis=0, concat_axis=0, tiled=True)
    asked = asked.reshape(peers * stride)

    swap = [(0, 1), (1, 0)]
    mate_ids = lax.ppermute(ids, "ah", swap)
    segments, bases, rel, past_slot, mine = plan_rows(
        place, ids, mate_ids, shard_rows, children, al_n, near, capacity, past_half
    )

    pairs = [(i, (i ^ s) if power else (i + s) % near) for s in range(near) for i in range(near)]
    steps = sorted(range(1, near), key=lambda s: (-bin(s).count("1"), -s))
    cuts = [0, 1 * near // 16, 5 * near // 16, 10 * near // 16, near - 1]
    waves = [steps[a:b] for a, b in zip(cuts, cuts[1:])]
    waves[-1] = waves[-1] + [0]
    slabs = [None] * near
    for number, wave in enumerate(waves):
        outs = gather_slabs(
            asked, place, node_table, wave, capacity, stride, past_half if number == 0 else 0, peers, al_n
        )
        if number == 0:
            past_out, outs = outs[0], outs[1:]
            past_in = lax.all_to_all(
                past_out.reshape(peers, 2 * past_half, width), AXES, split_axis=0, concat_axis=0, tiled=True
            ).reshape(peers * 2 * past_half, width)
        for shift, out in zip(wave, outs):
            slabs[shift] = lax.ppermute(out, HALF, pairs[shift * near : (shift + 1) * near]) if shift else out

    lanes = rounded(history, 128)
    past = arrange_past(past_slot, past_in, 2 * queries, history, lanes)
    own, lent = score_rows(segments, bases, rel, slabs, past, w_first, b_first, w_second, b_second, w_out.reshape(1, -1), history, lanes)
    back = lax.ppermute(lent, "ah", swap)
    return jnp.where(mine > 0, own, back)


def solution(mesh):
    pb_n, an_n = mesh.shape["pb"], mesh.shape["an"]
    fine = Mesh(mesh.devices.reshape(pb_n, 2, an_n // 2), AXES)
    rows = P(AXES, None)
    return jax.shard_map(
        body, mesh=fine, in_specs=(rows, rows, rows, P(), P(), P(), P(), P()), out_specs=rows, check_vma=False
    )
```

```python
import jax
import jax.numpy as jnp
from jax import lax
from jax.experimental import pallas as pl
from jax.experimental.pallas import tpu as pltpu
from jax.sharding import Mesh
from jax.sharding import PartitionSpec as P

AXES = ("pb", "ah", "al")
HALF = ("pb", "al")
BLOCK = 1024


def rounded(n, m):
    return -(-n // m) * m


def unroll_of(n, most=64):
    return max(u for u in range(1, most + 1) if n % u == 0)


VMEM = pl.BlockSpec(memory_space=pltpu.VMEM)
SMEM = pl.BlockSpec(memory_space=pltpu.SMEM)


def near_by(x):
    return pltpu.with_memory_space_constraint(x, pltpu.VMEM)


def widen(src, dst, rows, at=0, step=128):
    def go(i, c):
        dst[pl.ds(at + i * step, step), :] = src[pl.ds(i * step, step), :].astype(jnp.float32)
        return c

    step = unroll_of(rows // 8, step // 8) * 8
    lax.fori_loop(0, rows // step, go, 0)


def narrow(src, dst, rows, step=128):
    def go(i, c):
        dst[pl.ds(i * step, step), :] = src[pl.ds(i * step, step), :].astype(jnp.bfloat16)
        return c

    step = unroll_of(rows // 8, step // 8) * 8
    lax.fori_loop(0, rows // step, go, 0)


def split(ids, m):
    if m & (m - 1) == 0:
        return ids >> (m.bit_length() - 1), ids & (m - 1)
    return ids // m, ids % m


def iota(shape, axis):
    return lax.broadcasted_iota(jnp.int32, shape, axis)


def ones_where(mask):
    return jnp.where(mask, 1.0, 0.0).astype(jnp.bfloat16)


def exact_dot(a, b):
    return jnp.dot(a.astype(jnp.bfloat16), b.astype(jnp.bfloat16), preferred_element_type=jnp.float32)


def occurrences(keys, groups):
    rows, lanes = keys.shape
    hits = [keys == g for g in range(groups)]
    stack = jnp.concatenate([ones_where(hit) for hit in hits], axis=0)
    before = exact_dot(stack, ones_where(iota((lanes, lanes), 0) < iota((lanes, lanes), 1)))
    totals = exact_dot(stack, jnp.ones((lanes, 128), jnp.bfloat16))
    lane = iota((rows, 128), 1)
    counts = jnp.zeros((rows, 128), jnp.float32)
    for g in range(groups):
        counts = jnp.where(lane == g, totals[g * rows : (g + 1) * rows], counts)
    return hits, [before[g * rows : (g + 1) * rows] for g in range(groups)], counts


def places(hits, before, shifts):
    out = jnp.zeros(hits[0].shape, jnp.float32)
    for g, hit in enumerate(hits):
        out = jnp.where(hit, before[g] + shifts[:, g : g + 1], out)
    return out.astype(jnp.int32)


def build_lists(child_ids, history_ids, shard_rows, peers, capacity, past_half, stride):
    queries, children = child_ids.shape
    history = history_ids.shape[1]
    lanes = rounded(history, 128)
    digit_rows = rounded(2 * peers, 128)

    def kernel(kid_ref, past_ref, want_ref, ids_ref, pad, acc, spot_ref, digit_ref, *scratch):
        pad[...] = jnp.full(pad.shape, -1, jnp.int32)
        pad[:, :history] = past_ref[...]
        strict = ones_where(iota((queries, queries), 0) > iota((queries, queries), 1))
        for source, low, high, (owner_ref, rank_ref, off_ref) in (
            (kid_ref, 0, capacity, scratch[:3]),
            (pad, capacity, stride, scratch[3:]),
        ):
            owner, offset = split(source[...], shard_rows)
            hits, before, counts = occurrences(owner, peers)
            rank = places(hits, before, exact_dot(strict, counts))
            owner_ref[...] = owner
            rank_ref[...] = rank
            off_ref[...] = offset
            if low:
                ids_ref[:, children:] = owner * (2 * past_half) + rank
            else:
                ids_ref[:, :children] = source[...]
            size = source.shape[1]
            if digit_rows > 2 * peers:
                digit_ref[2 * peers :, :] = jnp.zeros((digit_rows - 2 * peers, digit_ref.shape[1]), jnp.bfloat16)

            def query(q, c, low=low, high=high, owner_ref=owner_ref, rank_ref=rank_ref, off_ref=off_ref, size=size):
                at = pl.ds(pl.multiple_of(q * size, size), size)
                hit = iota((peers, size), 0) == owner_ref[pl.ds(q, 1), :]
                offset = off_ref[pl.ds(q, 1), :].astype(jnp.float32)
                upper = jnp.floor(offset * (1.0 / 256.0))
                digit_ref[:peers, at] = jnp.where(hit, upper, 0.0).astype(jnp.bfloat16)
                digit_ref[peers : 2 * peers, at] = jnp.where(hit, offset - 256.0 * upper, 0.0).astype(jnp.bfloat16)
                spot_ref[: high - low, at] = ones_where(iota((high - low, size), 0) == rank_ref[pl.ds(q, 1), :])
                return c

            lax.fori_loop(0, queries, query, 0, unroll=2)
            acc[low:high, :] = lax.dot_general(
                spot_ref[: high - low, : queries * size],
                digit_ref[:, : queries * size],
                (((1,), (1,)), ((), ())),
                preferred_element_type=jnp.float32,
            )
        digits = acc[...].T.astype(jnp.int32)
        wanted = digits[:peers] * 256 + digits[peers : 2 * peers]
        for o in range(peers):
            want_ref[o, 0:1, :] = wanted[o : o + 1, :]

    return pl.pallas_call(
        kernel,
        out_shape=[
            jax.ShapeDtypeStruct((peers, 1, stride), jnp.int32),
            jax.ShapeDtypeStruct((queries, children + lanes), jnp.int32),
        ],
        in_specs=[VMEM, VMEM],
        out_specs=[VMEM, VMEM],
        scratch_shapes=[
            pltpu.VMEM((queries, lanes), jnp.int32),
            pltpu.VMEM((stride, digit_rows), jnp.float32),
            pltpu.VMEM((max(capacity, stride - capacity), queries * max(children, lanes)), jnp.bfloat16),
            pltpu.VMEM((digit_rows, queries * max(children, lanes)), jnp.bfloat16),
        ]
        + [pltpu.VMEM((queries, children), jnp.int32)] * 3
        + [pltpu.VMEM((queries, lanes), jnp.int32)] * 3,
        name="build_lists",
    )(child_ids, history_ids)


def plan_rows(here, ids, mate_ids, shard_rows, children, al_n, near, capacity, past_half):
    half = ids.shape[0]
    queries = 2 * half
    lanes = ids.shape[1] - children

    def kernel(here_ref, ids_ref, mate_ref, seg_ref, base_ref, rel_ref, slot_ref, mine_ref):
        at, side = here_ref[0], here_ref[1]
        kids = jnp.concatenate([ids_ref[:, :children], mate_ref[:, :children]], axis=0)
        owner, _ = split(kids, shard_rows)
        line, spot = split(owner, al_n)
        block, which_half = split(line, 2)
        local = block * al_n + spot
        part = (local ^ at) if near & (near - 1) == 0 else lax.rem(at - local + near, near)
        inside = which_half == side
        mine_ref[...] = inside.astype(jnp.int32)
        hits, before, counts = occurrences(jnp.where(inside, part, near), near)
        row, col = iota((queries, queries), 0), iota((queries, queries), 1)
        lower = row > col
        starts = exact_dot(ones_where(lower & ((row < half) == (col < half))), counts).astype(jnp.int32)
        square = (128, 128)
        offsets = exact_dot(counts, ones_where(iota(square, 0) < iota(square, 1)))
        lengths = exact_dot(counts, jnp.ones(square, jnp.bfloat16)).astype(jnp.int32)
        lengths = (lengths + 7) & -8
        bases = exact_dot(ones_where(lower), lengths.astype(jnp.float32)).astype(jnp.int32)
        rel_ref[...] = places(hits, before, offsets + (bases & 127).astype(jnp.float32))
        mate_rows = iota((queries, 128), 0) >= half
        seg_ref[:queries] = (
            iota((queries, 128), 1) * (2 * capacity) + jnp.where(mate_rows, capacity, 0) + starts
        )
        seg_ref[queries : 2 * queries] = bases + offsets.astype(jnp.int32)
        seg_ref[2 * queries :] = counts.astype(jnp.int32)
        base_ref[:queries] = bases
        base_ref[queries:] = jnp.broadcast_to((bases + lengths)[queries - 1 :], (8, 128))
        slot_ref[:half] = ids_ref[:, children:]
        slot_ref[half:] = mate_ref[:, children:] + past_half

    shapes = [(3 * queries, 128), (queries + 8, 128), (queries, children), (queries, lanes), (queries, children)]
    return pl.pallas_call(
        kernel,
        out_shape=[jax.ShapeDtypeStruct(shape, jnp.int32) for shape in shapes],
        in_specs=[SMEM, VMEM, VMEM],
        out_specs=[VMEM] * len(shapes),
        name="plan_rows",
    )(here, ids, near_by(mate_ids))


def gather_slabs(asked, here, table, shifts, capacity, stride, past_half, peers, al_n):
    width = table.shape[1]
    slab = 2 * capacity
    unroll = unroll_of(capacity)
    per = capacity // unroll

    def kernel(here_ref, asked_ref, table_ref, *rest):
        outs, wide, spare = rest[:-2], rest[-2], rest[-1]
        widen(table_ref, wide, table_ref.shape[0])
        if past_half:
            pasts, outs = outs[0], outs[1:]

            def past(d, c):
                at = d * stride + capacity
                rows = [wide[pl.ds(asked_ref[at + i], 1), :] for i in range(past_half)]
                mate = d + al_n * (1 - 2 * lax.rem(lax.div(d, al_n), 2))
                for i, row in enumerate(rows):
                    spare[pl.ds(d * 2 * past_half + i, 1), :] = row
                for i, row in enumerate(rows):
                    spare[pl.ds((mate * 2 + 1) * past_half + i, 1), :] = row
                return c

            lax.fori_loop(0, peers, past, 0)
            narrow(spare, pasts, peers * 2 * past_half)
        near = peers // 2
        at, side = here_ref[0], here_ref[1]
        for out, shift in zip(outs, shifts):
            target = (at ^ shift) if near & (near - 1) == 0 else lax.rem(at + shift, near)
            row = lax.div(target, al_n) * (2 * al_n) + lax.rem(target, al_n)
            own, mate = (row + side * al_n) * stride, (row + (1 - side) * al_n) * stride

            def child(t, c, own=own, mate=mate):
                at = jnp.where(t < per, own, mate - per * unroll) + t * unroll
                rows = [wide[pl.ds(asked_ref[at + i], 1), :] for i in range(unroll)]
                for i, row in enumerate(rows):
                    spare[pl.ds(t * unroll + i, 1), :] = row
                return c

            lax.fori_loop(0, 2 * per, child, 0)
            narrow(spare, out, slab)

    shapes = [jax.ShapeDtypeStruct((slab, width), jnp.bfloat16)] * len(shifts)
    spare_rows = slab
    if past_half:
        shapes = [jax.ShapeDtypeStruct((peers * 2 * past_half, width), jnp.bfloat16)] + shapes
        spare_rows = max(slab, peers * 2 * past_half)
    return pl.pallas_call(
        kernel,
        out_shape=shapes,
        in_specs=[SMEM, SMEM, VMEM],
        out_specs=[VMEM] * len(shapes),
        scratch_shapes=[
            pltpu.VMEM(table.shape, jnp.float32),
            pltpu.VMEM((spare_rows, width), jnp.float32),
        ],
        name="gather_past" if past_half else "gather_slabs",
    )(here, asked, table)


def arrange_past(slots, fetched, queries, history, lanes):
    rows, width = fetched.shape

    def kernel(slot_ref, in_ref, out_ref, wide, spare):
        widen(in_ref, wide, rows)
        spare[...] = jnp.zeros(spare.shape, jnp.float32)

        def one(q, c):
            for lo in range(0, history, 35):
                part = range(lo, min(lo + 35, history))
                vals = [wide[pl.ds(slot_ref[q, h], 1), :] for h in part]
                for h, val in zip(part, vals):
                    spare[pl.ds(h, 1), :] = val
            out_ref[pl.ds(pl.multiple_of(q * lanes, lanes), lanes), :] = spare[...].astype(jnp.bfloat16)
            return c

        lax.fori_loop(0, queries, one, 0)

    return pl.pallas_call(
        kernel,
        out_shape=jax.ShapeDtypeStruct((queries * lanes, width), fetched.dtype),
        in_specs=[SMEM, VMEM],
        out_specs=VMEM,
        scratch_shapes=[pltpu.VMEM((rows, width), jnp.float32), pltpu.VMEM((lanes, width), jnp.float32)],
        name="arrange_past",
    )(slots, near_by(fetched))


def score_rows(segments, bases, rel, mine, slabs, past, w_first, b_first, w_second, b_second, w_out, history, lanes):
    queries, children = rel.shape
    slab, width = slabs[0].shape
    parts = len(slabs)
    hidden = w_second.shape[0]
    batch = min(parts, 16)
    longest = rounded(queries * children + queries * 8, BLOCK)
    per_block = BLOCK // 128
    quick = 4
    group = 16
    half = queries // 2

    def kernel(seg_ref, base_ref, rel_ref, mine_ref, past_ref, w1, b1, w2, b2, wo, *rest):
        slab_refs, out_refs = rest[:parts], rest[parts : parts + 2]
        wide, rows, pool, line, g0, g1, g2 = rest[parts + 2 :]
        for i, ref in enumerate(slab_refs):
            widen(ref, wide, slab, at=i * slab)
        spots = [lax.broadcasted_iota(jnp.int32, (8, width), 0) + 8 * i for i in range(quick)]

        def segment(q, c):
            for x in range(0, parts, batch):
                src, dst, count = ([seg_ref[n * queries + q, x + i] for i in range(batch)] for n in range(3))
                chunks = [[wide[pl.ds(s + 8 * i, 8), :] for i in range(quick)] for s in src]
                for d, n, chunk in zip(dst, count, chunks):
                    for i, part in enumerate(chunk):
                        pltpu.store(rows.at[pl.ds(d + 8 * i, 8), :], part, mask=spots[i] < n)
                most = count[0]
                for n in count[1:]:
                    most = jnp.maximum(most, n)

                @pl.when(most > 8 * quick)
                def _(src=src, dst=dst, count=count):
                    for s, d, n in zip(src, dst, count):

                        def more(i, c, s=s, d=d, n=n):
                            pltpu.store(
                                rows.at[pl.ds(d + 8 * i, 8), :], wide[pl.ds(s + 8 * i, 8), :], mask=spots[0] < n - 8 * i
                            )
                            return c

                        lax.fori_loop(quick, (n + 7) >> 3, more, 0)

            return c

        lax.fori_loop(0, queries, segment, 0)

        def attend(g, c):
            for i in range(group):
                q = g * group + i
                base = pl.multiple_of(base_ref[q, 0], 8)
                kids = rows[pl.ds(base, children), :].astype(jnp.bfloat16)
                own = past_ref[pl.ds(pl.multiple_of(q * lanes, lanes), lanes), :]
                logits = lax.dot_general(kids, own, (((1,), (1,)), ((), ())), preferred_element_type=jnp.float32)
                logits = logits * width ** (-0.5)
                share = (jax.nn.sigmoid(logits) * history ** (-0.5)).astype(jnp.bfloat16)
                pool[pl.ds(base, children), :] = jnp.dot(share, own, preferred_element_type=jnp.float32)
            return c

        lax.fori_loop(0, queries // group, attend, 0)

        last = jnp.broadcast_to(wo[...], (8, hidden))

        def dense(b, c):
            at = pl.multiple_of(b * BLOCK, BLOCK)
            kids = rows[pl.ds(at, BLOCK), :].astype(jnp.bfloat16)
            pooled = pool[pl.ds(at, BLOCK), :].astype(jnp.bfloat16)
            joined = jnp.concatenate([kids, pooled], axis=1)
            first = jnp.dot(joined, w1[...], preferred_element_type=jnp.float32) + b1[...]
            first = jnp.maximum(first, 0.0).astype(jnp.bfloat16)
            second = jnp.dot(first, w2[...], preferred_element_type=jnp.float32) + b2[...]
            second = jnp.maximum(second, 0.0).astype(jnp.bfloat16)
            out = lax.dot_general(last, second, (((1,), (1,)), ((), ())), preferred_element_type=jnp.float32)
            for i in range(per_block):
                line[pl.ds(b * per_block + i, 1), :] = out[0:1, i * 128 : (i + 1) * 128]
            return c

        lax.fori_loop(0, (base_ref[queries, 0] + BLOCK - 1) // BLOCK, dense, 0)
        for q in range(queries):
            at = base_ref[q, 0] // 128
            for i, ref in enumerate((g0, g1, g2)):
                ref[q : q + 1, :] = line[pl.ds(at + i, 1), :]
        for q in range(0, queries, 8):
            for k in range(0, children, 128):
                spot = rel_ref[q : q + 8, k : k + 128]
                lane = spot & 127
                took = [jnp.take_along_axis(ref[q : q + 8, :], lane, axis=1) for ref in (g0, g1, g2)]
                out_ref, at = out_refs[q // half], q % half
                found = jnp.where(spot < 128, took[0], jnp.where(spot < 256, took[1], took[2]))
                here = mine_ref[q : q + 8, k : k + 128] > 0
                out_ref[at : at + 8, k : k + 128] = jnp.where(here, found, 0.0)

    wide_rows = parts * slab + 8 * quick
    return pl.pallas_call(
        kernel,
        out_shape=[jax.ShapeDtypeStruct((half, children), jnp.float32)] * 2,
        in_specs=[SMEM, SMEM] + [VMEM] * (8 + parts),
        out_specs=[VMEM] * 2,
        scratch_shapes=[
            pltpu.VMEM((wide_rows, width), jnp.float32),
            pltpu.VMEM((longest + children, width), jnp.float32),
            pltpu.VMEM((longest + children, width), jnp.float32),
            pltpu.VMEM((rounded(longest // 128 + 3, 8), 128), jnp.float32),
        ]
        + [pltpu.VMEM((queries, 128), jnp.float32)] * 3,
        name="score_rows",
    )(
        segments,
        bases,
        rel,
        mine,
        past,
        w_first,
        b_first.reshape(1, hidden),
        w_second,
        b_second.reshape(1, hidden),
        w_out,
        *slabs,
    )


def body(child_ids, history_ids, node_table, w_first, b_first, w_second, b_second, w_out):
    queries, children = child_ids.shape
    history = history_ids.shape[1]
    shard_rows, width = node_table.shape
    pb_n, al_n = lax.axis_size("pb"), lax.axis_size("al")
    peers, near = 2 * pb_n * al_n, pb_n * al_n
    pb, ah, al = (lax.axis_index(a) for a in AXES)
    place = jnp.stack([pb * al_n + al, ah])
    capacity = 5 * queries * children // (2 * peers)
    past_cap = (queries * history + peers - 1) // peers
    past_half = rounded(past_cap, 4)
    stride = rounded(capacity + past_half, 128)
    power = near & (near - 1) == 0

    wanted, ids = build_lists(child_ids, history_ids, shard_rows, peers, capacity, past_half, stride)
    asked = lax.all_to_all(wanted, AXES, split_axis=0, concat_axis=0, tiled=True)
    asked = asked.reshape(peers * stride)

    swap = [(0, 1), (1, 0)]
    mate_ids = lax.ppermute(ids, "ah", swap)
    segments, bases, rel, past_slot, mine = plan_rows(
        place, ids, mate_ids, shard_rows, children, al_n, near, capacity, past_half
    )

    pairs = [(i, (i ^ s) if power else (i + s) % near) for s in range(near) for i in range(near)]
    steps = sorted(range(1, near), key=lambda s: (-bin(s).count("1"), -s))
    cuts = [0, 1 * near // 16, 5 * near // 16, 10 * near // 16, near - 1]
    waves = [steps[a:b] for a, b in zip(cuts, cuts[1:])]
    waves[-1] = waves[-1] + [0]
    slabs = [None] * near
    for number, wave in enumerate(waves):
        outs = gather_slabs(
            asked, place, node_table, wave, capacity, stride, past_half if number == 0 else 0, peers, al_n
        )
        if number == 0:
            past_out, outs = outs[0], outs[1:]
            past_in = lax.all_to_all(
                past_out.reshape(peers, 2 * past_half, width), AXES, split_axis=0, concat_axis=0, tiled=True
            ).reshape(peers * 2 * past_half, width)
        for shift, out in zip(wave, outs):
            slabs[shift] = lax.ppermute(out, HALF, pairs[shift * near : (shift + 1) * near]) if shift else out

    lanes = rounded(history, 128)
    past = arrange_past(past_slot, past_in, 2 * queries, history, lanes)
    slabs = [near_by(x) if i in waves[-1] and i else x for i, x in enumerate(slabs)]
    own, lent = score_rows(segments, bases, rel, mine, slabs, past, w_first, b_first, w_second, b_second, w_out.reshape(1, -1), history, lanes)
    back = lax.ppermute(lent, "ah", swap)
    return own + back


def solution(mesh):
    pb_n, an_n = mesh.shape["pb"], mesh.shape["an"]
    fine = Mesh(mesh.devices.reshape(pb_n, 2, an_n // 2), AXES)
    rows = P(AXES, None)
    return jax.shard_map(
        body, mesh=fine, in_specs=(rows, rows, rows, P(), P(), P(), P(), P()), out_specs=rows, check_vma=False
    )
```

```python
import jax
import jax.numpy as jnp
from jax import lax
from jax.experimental import pallas as pl
from jax.experimental.pallas import tpu as pltpu
from jax.sharding import Mesh
from jax.sharding import PartitionSpec as P

AXES = ("pb", "ah", "al")
HALF = ("pb", "al")
BLOCK = 1280


def rounded(n, m):
    return -(-n // m) * m


def unroll_of(n, most=64):
    return max(u for u in range(1, most + 1) if n % u == 0)


VMEM = pl.BlockSpec(memory_space=pltpu.VMEM)
SMEM = pl.BlockSpec(memory_space=pltpu.SMEM)


def near_by(x):
    return pltpu.with_memory_space_constraint(x, pltpu.VMEM)


def widen(src, dst, rows, at=0, step=128):
    def go(i, c):
        dst[pl.ds(at + i * step, step), :] = src[pl.ds(i * step, step), :].astype(jnp.float32)
        return c

    step = unroll_of(rows // 8, step // 8) * 8
    lax.fori_loop(0, rows // step, go, 0)


def narrow(src, dst, rows, step=128):
    def go(i, c):
        dst[pl.ds(i * step, step), :] = src[pl.ds(i * step, step), :].astype(jnp.bfloat16)
        return c

    step = unroll_of(rows // 8, step // 8) * 8
    lax.fori_loop(0, rows // step, go, 0)


def split(ids, m):
    if m & (m - 1) == 0:
        return ids >> (m.bit_length() - 1), ids & (m - 1)
    return ids // m, ids % m


def iota(shape, axis):
    return lax.broadcasted_iota(jnp.int32, shape, axis)


def ones_where(mask):
    return jnp.where(mask, 1.0, 0.0).astype(jnp.bfloat16)


def exact_dot(a, b):
    return jnp.dot(a.astype(jnp.bfloat16), b.astype(jnp.bfloat16), preferred_element_type=jnp.float32)


def occurrences(keys, groups):
    rows, lanes = keys.shape
    hits = [keys == g for g in range(groups)]
    stack = jnp.concatenate([ones_where(hit) for hit in hits], axis=0)
    before = exact_dot(stack, ones_where(iota((lanes, lanes), 0) < iota((lanes, lanes), 1)))
    totals = exact_dot(stack, jnp.ones((lanes, 128), jnp.bfloat16))
    lane = iota((rows, 128), 1)
    counts = jnp.zeros((rows, 128), jnp.float32)
    for g in range(groups):
        counts = jnp.where(lane == g, totals[g * rows : (g + 1) * rows], counts)
    return hits, [before[g * rows : (g + 1) * rows] for g in range(groups)], counts


def places(hits, before, shifts):
    out = jnp.zeros(hits[0].shape, jnp.float32)
    for g, hit in enumerate(hits):
        out = jnp.where(hit, before[g] + shifts[:, g : g + 1], out)
    return out.astype(jnp.int32)


def build_lists(child_ids, history_ids, shard_rows, peers, capacity, past_half, stride):
    queries, children = child_ids.shape
    history = history_ids.shape[1]
    lanes = rounded(history, 128)
    digit_rows = rounded(2 * peers, 128)

    def kernel(kid_ref, past_ref, want_ref, ids_ref, pad, acc, spot_ref, digit_ref, *scratch):
        pad[...] = jnp.full(pad.shape, -1, jnp.int32)
        pad[:, :history] = past_ref[...]
        strict = ones_where(iota((queries, queries), 0) > iota((queries, queries), 1))
        for source, low, high, (owner_ref, rank_ref, off_ref) in (
            (kid_ref, 0, capacity, scratch[:3]),
            (pad, capacity, stride, scratch[3:]),
        ):
            owner, offset = split(source[...], shard_rows)
            hits, before, counts = occurrences(owner, peers)
            rank = places(hits, before, exact_dot(strict, counts))
            owner_ref[...] = owner
            rank_ref[...] = rank
            off_ref[...] = offset
            if low:
                ids_ref[:, children:] = owner * (2 * past_half) + rank
            else:
                ids_ref[:, :children] = source[...]
            size = source.shape[1]
            if digit_rows > 2 * peers:
                digit_ref[2 * peers :, :] = jnp.zeros((digit_rows - 2 * peers, digit_ref.shape[1]), jnp.bfloat16)

            def query(q, c, low=low, high=high, owner_ref=owner_ref, rank_ref=rank_ref, off_ref=off_ref, size=size):
                at = pl.ds(pl.multiple_of(q * size, size), size)
                hit = iota((peers, size), 0) == owner_ref[pl.ds(q, 1), :]
                offset = off_ref[pl.ds(q, 1), :].astype(jnp.float32)
                upper = jnp.floor(offset * (1.0 / 256.0))
                digit_ref[:peers, at] = jnp.where(hit, upper, 0.0).astype(jnp.bfloat16)
                digit_ref[peers : 2 * peers, at] = jnp.where(hit, offset - 256.0 * upper, 0.0).astype(jnp.bfloat16)
                spot_ref[: high - low, at] = ones_where(iota((high - low, size), 0) == rank_ref[pl.ds(q, 1), :])
                return c

            lax.fori_loop(0, queries, query, 0, unroll=2)
            acc[low:high, :] = lax.dot_general(
                spot_ref[: high - low, : queries * size],
                digit_ref[:, : queries * size],
                (((1,), (1,)), ((), ())),
                preferred_element_type=jnp.float32,
            )
        digits = acc[...].T.astype(jnp.int32)
        wanted = digits[:peers] * 256 + digits[peers : 2 * peers]
        for o in range(peers):
            want_ref[o, 0:1, :] = wanted[o : o + 1, :]

    return pl.pallas_call(
        kernel,
        out_shape=[
            jax.ShapeDtypeStruct((peers, 1, stride), jnp.int32),
            jax.ShapeDtypeStruct((queries, children + lanes), jnp.int32),
        ],
        in_specs=[VMEM, VMEM],
        out_specs=[VMEM, VMEM],
        scratch_shapes=[
            pltpu.VMEM((queries, lanes), jnp.int32),
            pltpu.VMEM((stride, digit_rows), jnp.float32),
            pltpu.VMEM((max(capacity, stride - capacity), queries * max(children, lanes)), jnp.bfloat16),
            pltpu.VMEM((digit_rows, queries * max(children, lanes)), jnp.bfloat16),
        ]
        + [pltpu.VMEM((queries, children), jnp.int32)] * 3
        + [pltpu.VMEM((queries, lanes), jnp.int32)] * 3,
        name="build_lists",
    )(child_ids, history_ids)


def plan_rows(here, ids, mate_ids, shard_rows, children, al_n, near, capacity, past_half):
    half = ids.shape[0]
    queries = 2 * half
    lanes = ids.shape[1] - children

    def kernel(here_ref, ids_ref, mate_ref, seg_ref, base_ref, rel_ref, slot_ref, mine_ref):
        at, side = here_ref[0], here_ref[1]
        kids = jnp.concatenate([ids_ref[:, :children], mate_ref[:, :children]], axis=0)
        owner, _ = split(kids, shard_rows)
        line, spot = split(owner, al_n)
        block, which_half = split(line, 2)
        local = block * al_n + spot
        part = (local ^ at) if near & (near - 1) == 0 else lax.rem(at - local + near, near)
        inside = which_half == side
        mine_ref[...] = inside.astype(jnp.int32)
        hits, before, counts = occurrences(jnp.where(inside, part, near), near)
        row, col = iota((queries, queries), 0), iota((queries, queries), 1)
        lower = row > col
        starts = exact_dot(ones_where(lower & ((row < half) == (col < half))), counts).astype(jnp.int32)
        square = (128, 128)
        offsets = exact_dot(counts, ones_where(iota(square, 0) < iota(square, 1)))
        lengths = exact_dot(counts, jnp.ones(square, jnp.bfloat16)).astype(jnp.int32)
        lengths = (lengths + 7) & -8
        bases = exact_dot(ones_where(lower), lengths.astype(jnp.float32)).astype(jnp.int32)
        rel_ref[...] = places(hits, before, offsets + (bases & 127).astype(jnp.float32))
        mate_rows = iota((queries, 128), 0) >= half
        seg_ref[:queries] = (
            iota((queries, 128), 1) * (2 * capacity) + jnp.where(mate_rows, capacity, 0) + starts
        )
        seg_ref[queries : 2 * queries] = bases + offsets.astype(jnp.int32)
        seg_ref[2 * queries :] = counts.astype(jnp.int32)
        base_ref[:queries] = bases
        base_ref[queries:] = jnp.broadcast_to((bases + lengths)[queries - 1 :], (8, 128))
        slot_ref[:half] = ids_ref[:, children:]
        slot_ref[half:] = mate_ref[:, children:] + past_half

    shapes = [(3 * queries, 128), (queries + 8, 128), (queries, children), (queries, lanes), (queries, children)]
    return pl.pallas_call(
        kernel,
        out_shape=[jax.ShapeDtypeStruct(shape, jnp.int32) for shape in shapes],
        in_specs=[SMEM, VMEM, VMEM],
        out_specs=[VMEM] * len(shapes),
        name="plan_rows",
    )(here, ids, near_by(mate_ids))


def gather_slabs(asked, here, table, shifts, capacity, stride, past_half, peers, al_n):
    width = table.shape[1]
    slab = 2 * capacity
    unroll = unroll_of(capacity)
    per = capacity // unroll

    def kernel(here_ref, asked_ref, table_ref, *rest):
        outs, wide, spare = rest[:-2], rest[-2], rest[-1]
        widen(table_ref, wide, table_ref.shape[0])
        if past_half:
            pasts, outs = outs[0], outs[1:]

            def past(d, c):
                at = d * stride + capacity
                rows = [wide[pl.ds(asked_ref[at + i], 1), :] for i in range(past_half)]
                mate = d + al_n * (1 - 2 * lax.rem(lax.div(d, al_n), 2))
                for i, row in enumerate(rows):
                    spare[pl.ds(d * 2 * past_half + i, 1), :] = row
                for i, row in enumerate(rows):
                    spare[pl.ds((mate * 2 + 1) * past_half + i, 1), :] = row
                return c

            lax.fori_loop(0, peers, past, 0)
            narrow(spare, pasts, peers * 2 * past_half)
        near = peers // 2
        at, side = here_ref[0], here_ref[1]
        for out, shift in zip(outs, shifts):
            target = (at ^ shift) if near & (near - 1) == 0 else lax.rem(at + shift, near)
            row = lax.div(target, al_n) * (2 * al_n) + lax.rem(target, al_n)
            own, mate = (row + side * al_n) * stride, (row + (1 - side) * al_n) * stride

            def child(t, c, own=own, mate=mate):
                at = jnp.where(t < per, own, mate - per * unroll) + t * unroll
                rows = [wide[pl.ds(asked_ref[at + i], 1), :] for i in range(unroll)]
                for i, row in enumerate(rows):
                    spare[pl.ds(t * unroll + i, 1), :] = row
                return c

            lax.fori_loop(0, 2 * per, child, 0)
            narrow(spare, out, slab)

    shapes = [jax.ShapeDtypeStruct((slab, width), jnp.bfloat16)] * len(shifts)
    spare_rows = slab
    if past_half:
        shapes = [jax.ShapeDtypeStruct((peers * 2 * past_half, width), jnp.bfloat16)] + shapes
        spare_rows = max(slab, peers * 2 * past_half)
    return pl.pallas_call(
        kernel,
        out_shape=shapes,
        in_specs=[SMEM, SMEM, VMEM],
        out_specs=[VMEM] * len(shapes),
        scratch_shapes=[
            pltpu.VMEM(table.shape, jnp.float32),
            pltpu.VMEM((spare_rows, width), jnp.float32),
        ],
        name="gather_past" if past_half else "gather_slabs",
    )(here, asked, table)


def arrange_past(slots, fetched, queries, history, lanes):
    rows, width = fetched.shape

    def kernel(slot_ref, in_ref, out_ref, wide, spare):
        widen(in_ref, wide, rows)
        spare[...] = jnp.zeros(spare.shape, jnp.float32)

        def one(q, c):
            for lo in range(0, history, 35):
                part = range(lo, min(lo + 35, history))
                vals = [wide[pl.ds(slot_ref[q, h], 1), :] for h in part]
                for h, val in zip(part, vals):
                    spare[pl.ds(h, 1), :] = val
            out_ref[pl.ds(pl.multiple_of(q * lanes, lanes), lanes), :] = spare[...].astype(jnp.bfloat16)
            return c

        lax.fori_loop(0, queries, one, 0)

    return pl.pallas_call(
        kernel,
        out_shape=pltpu.VMEM((queries * lanes, width), fetched.dtype),
        in_specs=[SMEM, VMEM],
        out_specs=VMEM,
        scratch_shapes=[pltpu.VMEM((rows, width), jnp.float32), pltpu.VMEM((lanes, width), jnp.float32)],
        name="arrange_past",
    )(slots, near_by(fetched))


def score_rows(segments, bases, rel, mine, slabs, past, w_first, b_first, w_second, b_second, w_out, history, lanes):
    queries, children = rel.shape
    slab, width = slabs[0].shape
    parts = len(slabs)
    hidden = w_second.shape[0]
    batch = min(parts, 16)
    longest = rounded(queries * children + queries * 8, BLOCK)
    per_block = BLOCK // 128
    quick = 4
    group = 32
    half = queries // 2

    def kernel(seg_ref, base_ref, rel_ref, mine_ref, past_ref, w1, b1, w2, b2, wo, *rest):
        slab_refs, out_refs = rest[:parts], rest[parts : parts + 2]
        wide, rows, pool, line, g0, g1, g2 = rest[parts + 2 :]
        for i, ref in enumerate(slab_refs):
            widen(ref, wide, slab, at=i * slab)
        spots = [lax.broadcasted_iota(jnp.int32, (8, width), 0) + 8 * i for i in range(quick)]

        def segment(q, c):
            for x in range(0, parts, batch):
                src, dst, count = ([seg_ref[n * queries + q, x + i] for i in range(batch)] for n in range(3))
                chunks = [[wide[pl.ds(s + 8 * i, 8), :] for i in range(quick)] for s in src]
                for d, n, chunk in zip(dst, count, chunks):
                    for i, part in enumerate(chunk):
                        pltpu.store(rows.at[pl.ds(d + 8 * i, 8), :], part, mask=spots[i] < n)
                most = count[0]
                for n in count[1:]:
                    most = jnp.maximum(most, n)

                @pl.when(most > 8 * quick)
                def _(src=src, dst=dst, count=count):
                    for s, d, n in zip(src, dst, count):

                        def more(i, c, s=s, d=d, n=n):
                            pltpu.store(
                                rows.at[pl.ds(d + 8 * i, 8), :], wide[pl.ds(s + 8 * i, 8), :], mask=spots[0] < n - 8 * i
                            )
                            return c

                        lax.fori_loop(quick, (n + 7) >> 3, more, 0)

            return c

        lax.fori_loop(0, queries, segment, 0)

        def attend(g, c):
            for i in range(group):
                q = g * group + i
                base = pl.multiple_of(base_ref[q, 0], 8)
                kids = rows[pl.ds(base, children), :].astype(jnp.bfloat16)
                own = past_ref[pl.ds(pl.multiple_of(q * lanes, lanes), lanes), :]
                logits = lax.dot_general(kids, own, (((1,), (1,)), ((), ())), preferred_element_type=jnp.float32)
                half_share = 0.5 * history ** (-0.5)
                share = (half_share + half_share * jnp.tanh(logits * (0.5 * width ** (-0.5)))).astype(jnp.bfloat16)
                pool[pl.ds(base, children), :] = jnp.dot(share, own, preferred_element_type=jnp.float32)
            return c

        lax.fori_loop(0, queries // group, attend, 0)

        last = jnp.broadcast_to(wo[...], (8, hidden))

        def dense(b, c):
            at = pl.multiple_of(b * BLOCK, BLOCK)
            kids = rows[pl.ds(at, BLOCK), :].astype(jnp.bfloat16)
            pooled = pool[pl.ds(at, BLOCK), :].astype(jnp.bfloat16)
            joined = jnp.concatenate([kids, pooled], axis=1)
            first = jnp.dot(joined, w1[...], preferred_element_type=jnp.float32) + b1[...]
            first = jnp.maximum(first, 0.0).astype(jnp.bfloat16)
            second = jnp.dot(first, w2[...], preferred_element_type=jnp.float32) + b2[...]
            second = jnp.maximum(second, 0.0).astype(jnp.bfloat16)
            out = lax.dot_general(last, second, (((1,), (1,)), ((), ())), preferred_element_type=jnp.float32)
            for i in range(per_block):
                line[pl.ds(b * per_block + i, 1), :] = out[0:1, i * 128 : (i + 1) * 128]
            return c

        lax.fori_loop(0, (base_ref[queries, 0] + BLOCK - 1) // BLOCK, dense, 0)
        for q in range(queries):
            at = base_ref[q, 0] // 128
            for i, ref in enumerate((g0, g1, g2)):
                ref[q : q + 1, :] = line[pl.ds(at + i, 1), :]
        for q in range(0, queries, 8):
            for k in range(0, children, 128):
                spot = rel_ref[q : q + 8, k : k + 128]
                lane = spot & 127
                took = [jnp.take_along_axis(ref[q : q + 8, :], lane, axis=1) for ref in (g0, g1, g2)]
                out_ref, at = out_refs[q // half], q % half
                found = jnp.where(spot < 128, took[0], jnp.where(spot < 256, took[1], took[2]))
                here = mine_ref[q : q + 8, k : k + 128] > 0
                out_ref[at : at + 8, k : k + 128] = jnp.where(here, found, 0.0)

    wide_rows = parts * slab + 8 * quick
    return pl.pallas_call(
        kernel,
        out_shape=[jax.ShapeDtypeStruct((half, children), jnp.float32)] * 2,
        in_specs=[SMEM, SMEM] + [VMEM] * (8 + parts),
        out_specs=[VMEM] * 2,
        scratch_shapes=[
            pltpu.VMEM((wide_rows, width), jnp.float32),
            pltpu.VMEM((longest + children, width), jnp.float32),
            pltpu.VMEM((longest + children, width), jnp.float32),
            pltpu.VMEM((rounded(longest // 128 + 3, 8), 128), jnp.float32),
        ]
        + [pltpu.VMEM((queries, 128), jnp.float32)] * 3,
        name="score_rows",
    )(
        segments,
        bases,
        rel,
        mine,
        near_by(past),
        w_first,
        b_first.reshape(1, hidden),
        w_second,
        b_second.reshape(1, hidden),
        w_out,
        *slabs,
    )


def body(child_ids, history_ids, node_table, w_first, b_first, w_second, b_second, w_out):
    queries, children = child_ids.shape
    history = history_ids.shape[1]
    shard_rows, width = node_table.shape
    pb_n, al_n = lax.axis_size("pb"), lax.axis_size("al")
    peers, near = 2 * pb_n * al_n, pb_n * al_n
    pb, ah, al = (lax.axis_index(a) for a in AXES)
    place = jnp.stack([pb * al_n + al, ah])
    capacity = 5 * queries * children // (2 * peers)
    past_cap = (queries * history + peers - 1) // peers
    past_half = rounded(past_cap, 4)
    stride = rounded(capacity + past_half, 128)
    power = near & (near - 1) == 0

    wanted, ids = build_lists(child_ids, history_ids, shard_rows, peers, capacity, past_half, stride)
    asked = lax.all_to_all(wanted, AXES, split_axis=0, concat_axis=0, tiled=True)
    asked = asked.reshape(peers * stride)

    swap = [(0, 1), (1, 0)]
    mate_ids = lax.ppermute(ids, "ah", swap)
    segments, bases, rel, past_slot, mine = plan_rows(
        place, ids, mate_ids, shard_rows, children, al_n, near, capacity, past_half
    )

    pairs = [(i, (i ^ s) if power else (i + s) % near) for s in range(near) for i in range(near)]
    steps = sorted(range(1, near), key=lambda s: (-bin(s).count("1"), -s))
    cuts = [0, 1 * near // 16, 5 * near // 16, 10 * near // 16, near - 1]
    waves = [steps[a:b] for a, b in zip(cuts, cuts[1:])]
    waves[-1] = waves[-1] + [0]
    slabs = [None] * near
    for number, wave in enumerate(waves):
        outs = gather_slabs(
            asked, place, node_table, wave, capacity, stride, past_half if number == 0 else 0, peers, al_n
        )
        if number == 0:
            past_out, outs = outs[0], outs[1:]
            past_in = lax.all_to_all(
                past_out.reshape(peers, 2 * past_half, width), AXES, split_axis=0, concat_axis=0, tiled=True
            ).reshape(peers * 2 * past_half, width)
        for shift, out in zip(wave, outs):
            slabs[shift] = lax.ppermute(out, HALF, pairs[shift * near : (shift + 1) * near]) if shift else out

    lanes = rounded(history, 128)
    past = arrange_past(past_slot, past_in, 2 * queries, history, lanes)
    slabs = [near_by(x) if i in waves[-1] and i else x for i, x in enumerate(slabs)]
    own, lent = score_rows(segments, bases, rel, mine, slabs, past, w_first, b_first, w_second, b_second, w_out.reshape(1, -1), history, lanes)
    back = lax.ppermute(lent, "ah", swap)
    return own + back


def solution(mesh):
    pb_n, an_n = mesh.shape["pb"], mesh.shape["an"]
    fine = Mesh(mesh.devices.reshape(pb_n, 2, an_n // 2), AXES)
    rows = P(AXES, None)
    return jax.shard_map(
        body, mesh=fine, in_specs=(rows, rows, rows, P(), P(), P(), P(), P()), out_specs=rows, check_vma=False
    )
```
